128 devices in a mesh: row: 8 (over z, x_lo), col: 16 (over x_hi, y, core).
Axes of the slice: x: 4 (x_hi: 2, x_lo: 2; x = x_hi * 2 + x_lo), y: 4, z: 4, core: 2. Of those that a mesh axis runs over, the one named last changes fastest.
Arguments:
- occupations: int32 [8192, 128], P('row'), may hold values from 0 to 2
- table: float32 [384, 1024], replicated, may hold values from -0.5 to 0.5
- weights: float32 [2, 1024, 4096], P(None, None, 'col'), may hold values from -0.1875 to 0.1875
- biases: float32 [2, 4096], P(None, 'col'), may hold values from -6 to 6
- heads: float32 [2, 4096], P(None, 'col'), may hold values from -18 to 18
- energies: float32 [8192], P('row'), may hold values from -6 to 6
Outputs:
- schur: float32 [8192, 8192], P('row', 'col')
- solved_rhs: float32 [8192], P('row')
The draws below stay inside these ranges and needn't reach their ends.
All inputs are finite; a program needn't handle non-finite values.
Results may differ from the reference program's by a relative error of at most 0.0034.
Values may be sent and summed in bfloat16 or wider, within the bound.
No kernel may reach another device: no remote copies, remote signals or barrier semaphores. Data moves between devices by JAX's collectives and lax.ppermute only.
A program may use at most 128 MiB of HBM per device.

```python
import math
import jax
import jax.numpy as jnp
from jax import lax

D = 1024
FF = 4096
ORB = 128
NSAMP = 8192
PANEL = 512


def draw_occupations(key, part):
    uniform_ints = jax.random.randint(jax.random.fold_in(key, 11), (NSAMP, ORB), 0, 1000)
    orbital_shift = jax.random.randint(jax.random.fold_in(key, 12), (ORB,), 0, 200)
    sample_ids = jnp.arange(NSAMP, dtype=jnp.int32)[:, None]
    threshold = 100 + 600 * sample_ids // NSAMP + orbital_shift[None, :]
    single = (uniform_ints < threshold).astype(jnp.int32)
    double = (uniform_ints < threshold // 3).astype(jnp.int32)
    return single + double


def block_levels(rng, shape, pieces, smallest, largest):
    def one(position, shards_of):
        heights = jax.random.uniform(jax.random.fold_in(jax.random.fold_in(rng, 6), position), (shards_of,), jnp.float32, smallest / len(pieces), largest / len(pieces))
        return jnp.repeat(jnp.exp(heights), shape[position] // shards_of).reshape((-1,) + (1,) * (len(shape) - position - 1))

    loudness = one(*pieces[0])
    for cut in pieces[1:]:
        loudness = loudness * one(*cut)
    return loudness


def centred(stream_key, dims, width, reach, split=(), held_as=jnp.bfloat16):
    level = block_levels(stream_key, dims, split, -0.22, 0.18) if split else 1.0
    entries = jax.random.normal(stream_key, dims, jnp.float32) * width * level
    return jnp.minimum(jnp.maximum(entries, -reach), reach).astype(held_as)


def setup_inputs(seed: int = 0) -> dict:
    seeds = jax.random.split(jax.random.key(seed), 7)
    return {
        "occupations": draw_occupations(jax.random.fold_in(seeds[6], 71), 0),
        "table": centred(seeds[1], (3 * ORB, D), ORB ** -0.5, 0.5, (), jnp.float32),
        "weights": centred(seeds[2], (2, D, FF), D ** -0.5, 0.1875, ((2, 16),), jnp.float32),
        "biases": centred(seeds[3], (2, FF), 1.0, 6.0, ((1, 16),), jnp.float32),
        "heads": centred(seeds[4], (2, FF), 3.0, 18.0, ((1, 16),), jnp.float32),
        "energies": centred(seeds[5], (NSAMP,), 1.0, 6.0, ((0, 8),), jnp.float32),
    }


norm_eps = 1e-06
diag_shift = 0.05

def jacobian(occupations, table, weights, biases, heads):
    onehot = jnp.concatenate([(occupations == 0).astype(jnp.float32), (occupations == 1).astype(jnp.float32), (occupations == 2).astype(jnp.float32)], axis=1)
    embedded = jnp.dot(onehot.astype(jnp.float32), table.astype(jnp.float32), precision=lax.Precision.HIGHEST, preferred_element_type=jnp.float32)
    embedded = embedded * lax.rsqrt(lax.optimization_barrier(jnp.mean(embedded * embedded, axis=-1, keepdims=True)) + norm_eps)
    blocks = []
    for panel_index in range(2):
        hidden = jnp.dot(embedded.astype(jnp.float32), weights[panel_index].astype(jnp.float32), precision=lax.Precision.HIGHEST, preferred_element_type=jnp.float32) + biases[panel_index]
        blocks.append(heads[panel_index] * jax.nn.sigmoid(hidden))
    return jnp.concatenate(blocks, axis=1)

def reference(occupations, table, weights, biases, heads, energies):
    derivs = jacobian(occupations, table, weights, biases, heads)
    sample_total = derivs.shape[0]
    centered = ((derivs - lax.optimization_barrier(jnp.sum(derivs, axis=0)) / sample_total) * (1.0 / math.sqrt(sample_total))).astype(jnp.bfloat16)
    kernel = jnp.dot(centered.astype(jnp.float32), centered.T.astype(jnp.float32), preferred_element_type=jnp.float32)
    kernel = kernel + diag_shift * jnp.eye(sample_total, dtype=jnp.float32)
    right_side = energies
    for panel_index in range(2):
        start = panel_index * PANEL
        diag_block = kernel[start:start + PANEL, start:start + PANEL]
        factor = jnp.linalg.cholesky(diag_block)
        column = kernel[:, start:start + PANEL]
        left_rows = lax.linalg.triangular_solve(factor, column, left_side=False, lower=True, transpose_a=True)
        kernel = kernel - jnp.dot(left_rows.astype(jnp.float32), left_rows.T.astype(jnp.float32), precision=lax.Precision.HIGHEST, preferred_element_type=jnp.float32)
        solved = lax.linalg.triangular_solve(factor, right_side[start:start + PANEL][:, None], left_side=True, lower=True)[:, 0]
        right_side = right_side - jnp.dot(left_rows.astype(jnp.float32), solved.astype(jnp.float32), precision=lax.Precision.HIGHEST, preferred_element_type=jnp.float32)
        right_side = right_side.at[start:start + PANEL].set(solved)
    return (kernel, right_side)
```

```python
import math

import jax
import jax.numpy as jnp
from jax import lax
from jax.experimental import pallas as pl
from jax.experimental.pallas import tpu as pltpu
from jax.sharding import Mesh
from jax.sharding import PartitionSpec as P

AXES = ("z", "xl", "xh", "y", "k")
SIZES = (4, 2, 2, 4, 2)
ROW = ("z", "xl")
COL = ("xh", "y", "k")
F32 = jnp.float32
BF16 = jnp.bfloat16


norm_eps = 1e-06
diag_shift = 0.05

NB = 128
PG = 16


def halves(x):
    hi = x.astype(BF16)
    return hi, (x - hi.astype(F32)).astype(BF16)


def dot3(a, b, dims=((1,), (0,))):
    (ah, al), (bh, bl) = a, b
    d = lambda u, v: lax.dot_general(u, v, (dims, ((), ())), preferred_element_type=F32)
    return d(ah, bh) + (d(ah, bl) + d(al, bh))


def factor_block(x_ref, f_ref, gh_ref, gl_ref):
    row = lax.broadcasted_iota(jnp.int32, (PG, NB), 0)
    lane = lax.broadcasted_iota(jnp.int32, (NB, NB), 1)
    for g in range(NB // PG):
        lo = g * PG
        p0 = x_ref[lo : lo + PG, :NB]
        p1 = x_ref[lo : lo + PG, NB:]
        cols = [jnp.broadcast_to(p0[:, lo + j : lo + j + 1], (PG, NB)) for j in range(PG)]
        f1 = jnp.zeros_like(p1)
        for i in range(PG):
            up = lambda v: jnp.broadcast_to(v[i : i + 1, :], (PG, NB))
            piv = up(cols[i])
            inv = 1.0 / piv
            here = row == i
            a1 = up(p1)
            f1 = jnp.where(here, a1 * lax.rsqrt(piv), f1)
            a0 = up(p0) * inv
            a1 = a1 * inv
            ci = cols[i]
            for j in range(i + 1, PG):
                b = up(cols[j]) * inv
                cols[j] = jnp.where(here, b, cols[j] - ci * b)
            p0 = jnp.where(here, a0, p0 - ci * a0)
            p1 = jnp.where(here, a1, p1 - ci * a1)
        f_ref[lo : lo + PG, :] = f1
        if g + 1 < NB // PG:
            for half, v in ((slice(0, NB), p0), (slice(NB, 2 * NB), p1)):
                gh_ref[lo : lo + PG, half], gl_ref[lo : lo + PG, half] = halves(v)
            rest = slice(lo + PG, NB)
            n = NB - lo - PG
            inside = (lane[:n] >= lo) & (lane[:n] < lo + PG)
            left = halves(jnp.where(inside, x_ref[rest, :NB], 0.0))
            x_ref[rest, :] = x_ref[rest, :] - dot3(left, (gh_ref[...], gl_ref[...]))


def eliminate(t_ref, w_ref, first, x_ref, f_ref, gh_ref, gl_ref, yh_ref, yl_ref):
    n = t_ref.shape[1]
    gh_ref[...] = jnp.zeros_like(gh_ref)
    gl_ref[...] = jnp.zeros_like(gl_ref)
    eye = lax.broadcasted_iota(jnp.int32, (NB, NB), 0) == lax.broadcasted_iota(jnp.int32, (NB, NB), 1)
    ident = eye.astype(F32)
    wide = lax.broadcasted_iota(jnp.int32, (NB, n), 1)

    def step(b, carry):
        at = pl.multiple_of(first + b * NB, NB)
        mine = pl.ds(pl.multiple_of(b * NB, NB), NB)
        here = pl.ds(at, NB)
        x_ref[:, :NB] = t_ref[mine, here] + diag_shift * ident
        x_ref[:, NB:] = ident
        factor_block(x_ref, f_ref, gh_ref, gl_ref)
        linv = halves(f_ref[...])
        t_ref[mine, here] = ident
        y = dot3(linv, halves(t_ref[mine, :]))
        w_ref[mine, :] = jnp.where(wide < at + NB, y, 0.0)
        yh_ref[...], yl_ref[...] = halves(y)

        def below(r, c):
            rows = pl.ds(pl.multiple_of(r * NB, NB), NB)
            mult = dot3(halves(t_ref[rows, here]), linv, ((1,), (1,)))
            t_ref[rows, here] = jnp.zeros((NB, NB), F32)
            t_ref[rows, :] = t_ref[rows, :] - dot3(halves(mult), (yh_ref[...], yl_ref[...]))
            return c

        lax.fori_loop(b + 1, t_ref.shape[0] // NB, below, 0)
        return carry

    lax.fori_loop(0, w_ref.shape[0] // NB, step, 0)


def first_half(*refs):
    parts, (w_ref, out_ref, t_ref, *scratch, sems) = refs[:8], refs[8:]
    z, k = lax.axis_index("z"), lax.axis_index("k")
    copies = []
    for dk in range(2):
        for dz in range(4):
            i = dk * 4 + dz
            at = ((k + dk) % 2) * 512 + ((z + dz) % 4) * 128
            copies.append(pltpu.make_async_copy(parts[i], t_ref.at[pl.ds(pl.multiple_of(at, 128), 128)], sems.at[i]))
    for c in copies:
        c.start()
    for c in copies:
        c.wait()
    eliminate(t_ref, w_ref, 0, *scratch)
    out_ref[...] = t_ref[512:, :]


def later_part(first, a_ref, w_ref, *refs):
    done = w_ref.shape[0]
    (out_ref,), (t_ref, *scratch) = (refs[:1], refs[1:]) if first + done < 1024 else ((None,), refs)
    t_ref[...] = a_ref[...]
    eliminate(t_ref, w_ref, first, *scratch)
    if out_ref is not None:
        out_ref[...] = t_ref[done:, :]


FACTOR_SCRATCH = [
    pltpu.VMEM((NB, 2 * NB), F32),
    pltpu.VMEM((NB, NB), F32),
    pltpu.VMEM((NB, 2 * NB), BF16),
    pltpu.VMEM((NB, 2 * NB), BF16),
    pltpu.VMEM((NB, 1024), BF16),
    pltpu.VMEM((NB, 1024), BF16),
]
KERNEL_PARAMS = pltpu.CompilerParams(vmem_limit_bytes=40 * 1024 * 1024)


def factor_cost(flops):
    return pl.CostEstimate(flops=flops, transcendentals=0, bytes_accessed=8_000_000)


def lines(n):
    return jax.ShapeDtypeStruct((n, 1024), F32)


def start_inverse(parts):
    return pl.pallas_call(
        first_half,
        out_shape=(lines(512), lines(512)),
        in_specs=[pl.BlockSpec(memory_space=pl.ANY)] * 8,
        scratch_shapes=[pltpu.VMEM((1024, 1024), F32), *FACTOR_SCRATCH, pltpu.SemaphoreType.DMA((8,))],
        compiler_params=KERNEL_PARAMS,
        cost_estimate=factor_cost(15_000_000_000),
        name="inverse_first",
    )(*parts)


def go_on_inverse(rest, count):
    left = rest.shape[0]
    return pl.pallas_call(
        lambda *refs: later_part(1024 - left, *refs),
        out_shape=(lines(count), lines(left - count)) if left > count else (lines(count),),
        scratch_shapes=[pltpu.VMEM((left, 1024), F32), *FACTOR_SCRATCH],
        compiler_params=KERNEL_PARAMS,
        cost_estimate=factor_cost(5_000_000_000),
    )(rest)


def block_kernel(far, halves_in, across, down, acc, outs, a_ref, b_ref, sems):
    z, xl, xh, y, k = [lax.axis_index(a) for a in AXES]
    wanted = lambda d: ((d % 4 == (y + 2) % 4) | (d // 2 == (z + 2) % 4)) == far
    copies = []
    for i in range(8):
        step, flip = i % 4, i // 4
        if across[i] is not None:
            d = ((xh + flip) % 2) * 4 + (y + step) % 4
            copies.append((d, pltpu.make_async_copy(across[i], a_ref.at[d], sems.at[0, i])))
        if down[i] is not None:
            d = ((z + step) % 4) * 2 + (xl + flip) % 2
            src = down[i]
            if len(halves_in) == 1:
                src = src.at[pl.ds(pl.multiple_of(((k + halves_in[0]) % 2) * 512, 512), 512)]
            copies.append((d, pltpu.make_async_copy(src, b_ref.at[d], sems.at[1, i])))
    for d, c in copies:
        pl.when(wanted(d))(c.start)
    for o in range(len(outs)):
        outs[o][...] = acc[o][...] if acc else jnp.zeros_like(outs[o])
    for d, c in copies:
        pl.when(wanted(d))(c.wait)

    def one(d, carry):
        @pl.when(wanted(d))
        def _():
            for o, theirs in enumerate(halves_in):
                at = pl.multiple_of(((k + theirs) % 2) * 512, 512) if len(halves_in) == 2 else 0
                b = b_ref[d, pl.ds(at, 512), :]
                for r in range(0, 1024, 256):
                    outs[o][r : r + 256, :] += outer(a_ref[d, r : r + 256, :], b)

        return carry

    lax.fori_loop(0, 8, one, 0)


BLOCK = jax.ShapeDtypeStruct((1024, 512), F32)


def near_product(across, down):
    ids = [0, 1, 3, 4, 5, 7]

    def body(*refs):
        a, b = [None] * 8, [None] * 8
        for n, i in enumerate(ids):
            a[i], b[i] = refs[n], refs[6 + n]
        block_kernel(False, (1, 0), a, b, (), refs[12:14], *refs[14:])

    return pl.pallas_call(
        body,
        out_shape=(BLOCK, BLOCK),
        in_specs=[pl.BlockSpec(memory_space=pl.ANY)] * 12,
        scratch_shapes=[
            pltpu.VMEM((8, 1024, 512), BF16),
            pltpu.VMEM((8, 1024, 512), BF16),
            pltpu.SemaphoreType.DMA((2, 8)),
        ],
        compiler_params=KERNEL_PARAMS,
        cost_estimate=pl.CostEstimate(flops=4_300_000_000, transcendentals=0, bytes_accessed=14_000_000),
        name="block_near",
    )(*[across[i] for i in ids], *[down[i] for i in ids])


def far_product(across, down, acc, theirs):
    def body(*refs):
        block_kernel(True, (theirs,), refs[:8], refs[8:16], refs[16:17], refs[17:18], *refs[18:])

    return pl.pallas_call(
        body,
        out_shape=BLOCK,
        in_specs=[pl.BlockSpec(memory_space=pl.ANY)] * 16 + [pl.BlockSpec(memory_space=pltpu.VMEM)],
        scratch_shapes=[
            pltpu.VMEM((8, 1024, 512), BF16),
            pltpu.VMEM((8, 512, 512), BF16),
            pltpu.SemaphoreType.DMA((2, 8)),
        ],
        compiler_params=KERNEL_PARAMS,
        cost_estimate=pl.CostEstimate(flops=2_200_000_000, transcendentals=0, bytes_accessed=8_000_000),
        name="block_far_theirs" if theirs else "block_far_own",
    )(*across, *down, acc)


def swap(x, axis):
    return lax.ppermute(x, axis, [(0, 1), (1, 0)])


def shift(x, axis, by):
    n = lax.axis_size(axis)
    return lax.ppermute(x, axis, [(i, (i + by) % n) for i in range(n)])


def send(x, axis, src, dst):
    return lax.ppermute(x, axis, [(src, dst)])


def after(x, *others):
    return lax.optimization_barrier((x, *others))[0]


def gather2(x, axis):
    other = swap(x, axis)
    first = lax.axis_index(axis) == 0
    return jnp.stack([jnp.where(first, x, other), jnp.where(first, other, x)])


def ring4(x, axis):
    return [x, shift(x, axis, -1), shift(x, axis, 2), shift(x, axis, 1)]


def in_order(parts, axis):
    turn = (4 - lax.axis_index(axis)) % 4
    twice = jnp.concatenate(parts + parts[:3])
    size = parts[0].shape[0]
    return lax.dynamic_slice_in_dim(twice, turn * size, 4 * size)


def scatter2(x, axis):
    me = lax.axis_index(axis)
    other = swap(lax.dynamic_index_in_dim(x, 1 - me, 0, False), axis)
    return lax.dynamic_index_in_dim(x, me, 0, False) + other


def scatter4(x, axis):
    me = lax.axis_index(axis)
    pick = lambda ahead: lax.dynamic_index_in_dim(x, (me + ahead) % 4, 0, False)
    return (pick(0) + shift(pick(2), axis, 2)) + (shift(pick(1), axis, 1) + shift(pick(3), axis, -1))


def first_of_pair(x):
    return jnp.where(lax.axis_index("xl") == 0, x, send(x, "xl", 0, 1))


def first_of_ring(x):
    return lax.select_n(lax.axis_index("z"), x, send(x, "z", 0, 1), send(x, "z", 0, 2), send(x, "z", 0, 3))


def transpose_chips(x):
    pairs = []
    for d in range(math.prod(SIZES)):
        k, c, r = d % 2, (d // 2) % 8, d // 16
        pairs.append((d, (c * 8 + r) * 2 + k))
    return lax.ppermute(x, AXES, pairs)


def sum_rows(x):
    x = x + swap(x, "xl")
    x = x + lax.ppermute(x, "z", [(i, i ^ 1) for i in range(4)])
    return x + lax.ppermute(x, "z", [(i, i ^ 2) for i in range(4)])


def embed(occupations, table):
    onehot = jnp.concatenate([(occupations == v).astype(F32) for v in range(3)], axis=1)
    embedded = jnp.dot(onehot, table, precision=lax.Precision.HIGH, preferred_element_type=F32)
    return embedded * lax.rsqrt(jnp.mean(embedded * embedded, axis=-1, keepdims=True) + norm_eps)


def log_derivatives(embedded, weights, biases, heads):
    blocks = []
    for p in range(2):
        hidden = jnp.dot(embedded, weights[p], precision=lax.Precision.HIGH, preferred_element_type=F32) + biases[p]
        blocks.append(heads[p] * jax.nn.sigmoid(hidden))
    return jnp.concatenate(blocks, axis=1)


def outer(a, b):
    return lax.dot_general(a, b, (((1,), (1,)), ((), ())), preferred_element_type=F32)


def outer3(a, b):
    return lax.dot_general(
        a, b, (((1,), (1,)), ((), ())), precision=lax.Precision.HIGH, preferred_element_type=F32
    )


def on_device(occupations, table, weights, biases, heads, energies):
    rows = occupations.shape[0]
    total = rows * 8
    cols = total // 16
    z, xl, xh, y, core = [lax.axis_index(a) for a in AXES]
    row, chip_col = z * 2 + xl, xh * 4 + y
    par = weights.shape[0] * weights.shape[2]

    pair_occ = first_of_pair(occupations.astype(BF16))
    embedded = after(embed(occupations, table), pair_occ)
    first_occ = first_of_ring(pair_occ)
    derivs = log_derivatives(embedded, weights, biases, heads)
    sums = jnp.sum(derivs, axis=0, keepdims=True)
    first_derivs = log_derivatives(embed(after(first_occ, sums), table), weights, biases, heads)
    mean = sum_rows(sums) / total
    center = lambda d: ((d - mean) * (1.0 / math.sqrt(total))).astype(BF16)
    own, first = center(derivs), center(first_derivs)

    eye = lambda r, c, r0, c0: jnp.where(
        (lax.broadcasted_iota(jnp.int32, (r, c), 0) + r0) == (lax.broadcasted_iota(jnp.int32, (r, c), 1) + c0),
        diag_shift,
        0.0,
    ).astype(F32)

    pick = first.reshape(2, 4, 4, 2, 16, par)
    pick = lax.dynamic_index_in_dim(lax.dynamic_index_in_dim(pick, z, 1, False), xl, 2, False)
    slab = outer(pick.reshape(128, par), first).reshape(2, 4, 2, 8, rows)
    own_x = after(own, slab)
    turned = transpose_chips(own_x)
    slab = scatter2(slab, "k")
    panel = outer(after(own, slab), first).reshape(2, 4, 2, rows // 16, rows)
    slab = scatter4(slab, "y")
    panel = scatter2(after(panel, slab), "k")
    slab = scatter2(slab, "xh")
    slab = gather2(gather2(slab, "xh"), "xl")
    beside = swap(after(own, slab), "xh")
    slab = in_order(ring4(slab.reshape(32, rows), "y"), "y")
    panel = scatter4(after(panel, slab), "y")
    own_y = after(own, slab)
    own_next, own_prev = shift(own_y, "y", -1), shift(own_y, "y", 1)
    parts = ring4(slab, "z")
    parts = parts + [swap(p, "k") for p in parts]
    turned, beside, *parts = lax.optimization_barrier((turned, beside, *parts))
    side_next, side_prev = shift(beside, "y", -1), shift(beside, "y", 1)
    turned_next, turned_prev = shift(turned, "z", -1), shift(turned, "z", 1)
    turned_side = swap(turned, "xl")

    low, rest = start_inverse(parts)
    panel, own_prev, turned_prev, turned_side, rest = lax.optimization_barrier(
        (panel, own_prev, turned_prev, turned_side, rest)
    )
    panel = scatter2(panel, "xh")
    tside_next, tside_prev = shift(turned_side, "z", -1), shift(turned_side, "z", 1)
    own_far = shift(own_prev, "y", 1)
    turned_far = shift(turned_prev, "z", 1)

    mid, rest = go_on_inverse(rest, 256)
    panel, side_next, rest = lax.optimization_barrier((panel, side_next, rest))
    mine = gather2(panel, "xh").reshape(rows // 8, rows)
    panel_turned = transpose_chips(panel)

    (high,) = go_on_inverse(rest, 256)
    mine, panel_turned, side_next, high = lax.optimization_barrier((mine, panel_turned, side_next, high))

    mine = ring4(mine, "y")
    other = ring4(gather2(panel_turned, "xl").reshape(rows // 8, rows), "z")
    side_far = shift(side_next, "y", -1)
    tside_far = shift(tside_next, "z", -1)
    across = [own, own_next, own_far, own_prev, beside, side_next, side_far, side_prev]
    down = [turned, turned_next, turned_far, turned_prev, turned_side, tside_next, tside_far, tside_prev]
    acc_theirs, acc_own = near_product(across, down)

    mine = gather2(in_order(mine, "y"), "k").reshape(rows, rows)
    other = in_order(other, "z").reshape(2, 4, rows // 16, rows).transpose(1, 0, 2, 3).reshape(cols, rows)
    mine = mine + eye(rows, rows, row * rows, 0)
    other = other + eye(cols, rows, chip_col * rows + core * cols, 0)
    inverse = [low[:, :512], mid[:, :768], high]
    left = jnp.concatenate([outer3(mine[:, : w.shape[1]], w) for w in inverse], 1)
    right = jnp.concatenate([outer3(other[:, : w.shape[1]], w) for w in inverse], 1)
    first_side = first_of_ring(first_of_pair(after(energies.reshape(8, -1), high))).reshape(1, -1)
    exact = lambda a, b: lax.dot_general(
        a, b, (((1,), (1,)), ((), ())), precision=lax.Precision.HIGHEST, preferred_element_type=F32
    )
    solved = jnp.concatenate([exact(first_side[:, : w.shape[1]], w) for w in inverse], 1)
    side = energies - jnp.sum(left * solved, axis=1)
    side = jnp.where(row == 0, solved[0], side)
    update = outer3(left, right) - eye(rows, cols, row * rows, chip_col * rows + core * cols)

    theirs = swap(far_product(across, down, acc_theirs, 1), "k")
    schur = (far_product(across, down, acc_own, 0) + theirs) - update
    return schur, side


def solution(mesh):
    torus = Mesh(mesh.devices.reshape(SIZES), AXES)
    placed = (P(ROW, None), P(), P(None, None, COL), P(None, COL), P(None, COL), P(ROW))


    return jax.shard_map(on_device, mesh=torus, in_specs=placed, out_specs=(P(ROW, COL), P(ROW)), check_vma=False)
```

```python
import math

import jax
import jax.numpy as jnp
from jax import lax
from jax.experimental import pallas as pl
from jax.experimental.pallas import tpu as pltpu
from jax.sharding import Mesh
from jax.sharding import PartitionSpec as P

AXES = ("z", "xl", "xh", "y", "k")
SIZES = (4, 2, 2, 4, 2)
ROW = ("z", "xl")
COL = ("xh", "y", "k")
F32 = jnp.float32
BF16 = jnp.bfloat16


norm_eps = 1e-06
diag_shift = 0.05

NB = 128
PG = 16


def halves(x):
    hi = x.astype(BF16)
    return hi, (x - hi.astype(F32)).astype(BF16)


def dot3(a, b, dims=((1,), (0,))):
    (ah, al), (bh, bl) = a, b
    d = lambda u, v: lax.dot_general(u, v, (dims, ((), ())), preferred_element_type=F32)
    return d(ah, bh) + (d(ah, bl) + d(al, bh))


def factor_block(x_ref, f_ref, gh_ref, gl_ref):
    row = lax.broadcasted_iota(jnp.int32, (PG, NB), 0)
    lane = lax.broadcasted_iota(jnp.int32, (NB, NB), 1)
    for g in range(NB // PG):
        lo = g * PG
        p0 = x_ref[lo : lo + PG, :NB]
        p1 = x_ref[lo : lo + PG, NB:]
        cols = [jnp.broadcast_to(p0[:, lo + j : lo + j + 1], (PG, NB)) for j in range(PG)]
        f1 = jnp.zeros_like(p1)
        for i in range(PG):
            up = lambda v: jnp.broadcast_to(v[i : i + 1, :], (PG, NB))
            piv = up(cols[i])
            inv = 1.0 / piv
            here = row == i
            a1 = up(p1)
            f1 = jnp.where(here, a1 * lax.rsqrt(piv), f1)
            a0 = up(p0) * inv
            a1 = a1 * inv
            ci = cols[i]
            for j in range(i + 1, PG):
                b = up(cols[j]) * inv
                cols[j] = jnp.where(here, b, cols[j] - ci * b)
            p0 = jnp.where(here, a0, p0 - ci * a0)
            p1 = jnp.where(here, a1, p1 - ci * a1)
        f_ref[lo : lo + PG, :] = f1
        if g + 1 < NB // PG:
            for half, v in ((slice(0, NB), p0), (slice(NB, 2 * NB), p1)):
                gh_ref[lo : lo + PG, half], gl_ref[lo : lo + PG, half] = halves(v)
            rest = slice(lo + PG, NB)
            n = NB - lo - PG
            inside = (lane[:n] >= lo) & (lane[:n] < lo + PG)
            left = halves(jnp.where(inside, x_ref[rest, :NB], 0.0))
            x_ref[rest, :] = x_ref[rest, :] - dot3(left, (gh_ref[...], gl_ref[...]))


def eliminate(t_ref, w_ref, first, x_ref, f_ref, gh_ref, gl_ref, yh_ref, yl_ref):
    n = t_ref.shape[1]
    gh_ref[...] = jnp.zeros_like(gh_ref)
    gl_ref[...] = jnp.zeros_like(gl_ref)
    eye = lax.broadcasted_iota(jnp.int32, (NB, NB), 0) == lax.broadcasted_iota(jnp.int32, (NB, NB), 1)
    ident = eye.astype(F32)
    wide = lax.broadcasted_iota(jnp.int32, (NB, n), 1)

    def step(b, carry):
        at = pl.multiple_of(first + b * NB, NB)
        mine = pl.ds(pl.multiple_of(b * NB, NB), NB)
        here = pl.ds(at, NB)
        x_ref[:, :NB] = t_ref[mine, here] + diag_shift * ident
        x_ref[:, NB:] = ident
        factor_block(x_ref, f_ref, gh_ref, gl_ref)
        linv = halves(f_ref[...])
        t_ref[mine, here] = ident
        y = dot3(linv, halves(t_ref[mine, :]))
        w_ref[mine, :] = jnp.where(wide < at + NB, y, 0.0)
        yh_ref[...], yl_ref[...] = halves(y)

        def below(r, c):
            rows = pl.ds(pl.multiple_of(r * NB, NB), NB)
            mult = dot3(halves(t_ref[rows, here]), linv, ((1,), (1,)))
            t_ref[rows, here] = jnp.zeros((NB, NB), F32)
            t_ref[rows, :] = t_ref[rows, :] - dot3(halves(mult), (yh_ref[...], yl_ref[...]))
            return c

        lax.fori_loop(b + 1, t_ref.shape[0] // NB, below, 0)
        return carry

    lax.fori_loop(0, w_ref.shape[0] // NB, step, 0)


def first_half(*refs):
    parts, (w_ref, out_ref, t_ref, *scratch, sems) = refs[:8], refs[8:]
    z, k = lax.axis_index("z"), lax.axis_index("k")
    copies = []
    for dk in range(2):
        for dz in range(4):
            i = dk * 4 + dz
            at = ((k + dk) % 2) * 512 + ((z + dz) % 4) * 128
            copies.append(pltpu.make_async_copy(parts[i], t_ref.at[pl.ds(pl.multiple_of(at, 128), 128)], sems.at[i]))
    for c in copies:
        c.start()
    for c in copies:
        c.wait()
    eliminate(t_ref, w_ref, 0, *scratch)
    out_ref[...] = t_ref[512:, :]


def later_part(first, a_ref, w_ref, *refs):
    done = w_ref.shape[0]
    (out_ref,), (t_ref, *scratch) = (refs[:1], refs[1:]) if first + done < 1024 else ((None,), refs)
    t_ref[...] = a_ref[...]
    eliminate(t_ref, w_ref, first, *scratch)
    if out_ref is not None:
        out_ref[...] = t_ref[done:, :]


FACTOR_SCRATCH = [
    pltpu.VMEM((NB, 2 * NB), F32),
    pltpu.VMEM((NB, NB), F32),
    pltpu.VMEM((NB, 2 * NB), BF16),
    pltpu.VMEM((NB, 2 * NB), BF16),
    pltpu.VMEM((NB, 1024), BF16),
    pltpu.VMEM((NB, 1024), BF16),
]
KERNEL_PARAMS = pltpu.CompilerParams(vmem_limit_bytes=40 * 1024 * 1024)


def factor_cost(flops):
    return pl.CostEstimate(flops=flops, transcendentals=0, bytes_accessed=8_000_000)


def lines(n):
    return jax.ShapeDtypeStruct((n, 1024), F32)


def start_inverse(parts):
    return pl.pallas_call(
        first_half,
        out_shape=(lines(512), lines(512)),
        in_specs=[pl.BlockSpec(memory_space=pl.ANY)] * 8,
        scratch_shapes=[pltpu.VMEM((1024, 1024), F32), *FACTOR_SCRATCH, pltpu.SemaphoreType.DMA((8,))],
        compiler_params=KERNEL_PARAMS,
        cost_estimate=factor_cost(15_000_000_000),
        name="inverse_first",
    )(*parts)


def go_on_inverse(rest, count):
    left = rest.shape[0]
    return pl.pallas_call(
        lambda *refs: later_part(1024 - left, *refs),
        out_shape=(lines(count), lines(left - count)) if left > count else (lines(count),),
        scratch_shapes=[pltpu.VMEM((left, 1024), F32), *FACTOR_SCRATCH],
        compiler_params=KERNEL_PARAMS,
        cost_estimate=factor_cost(5_000_000_000),
    )(rest)


def block_kernel(far, across, down, outs, a_ref, b_ref, sems):
    z, xl, xh, y, k = [lax.axis_index(a) for a in AXES]
    wanted = lambda d: ((d % 4 == (y + 2) % 4) | (d // 2 == (z + 2) % 4)) == far
    copies = []
    for i in range(8):
        step, flip = i % 4, i // 4
        if across[i] is not None:
            d = ((xh + flip) % 2) * 4 + (y + step) % 4
            copies.append((d, pltpu.make_async_copy(across[i], a_ref.at[d], sems.at[0, i])))
            d = ((z + step) % 4) * 2 + (xl + flip) % 2
            copies.append((d, pltpu.make_async_copy(down[i], b_ref.at[d], sems.at[1, i])))
    for d, c in copies:
        pl.when(wanted(d))(c.start)
    for out in outs:
        out[...] = jnp.zeros_like(out)
    for d, c in copies:
        pl.when(wanted(d))(c.wait)

    def one(d, carry):
        @pl.when(wanted(d))
        def _():
            for theirs, out in zip((1, 0), outs):
                b = b_ref[d, pl.ds(pl.multiple_of(((k + theirs) % 2) * 512, 512), 512), :]
                for r in range(0, 1024, 256):
                    out[r : r + 256, :] += outer(a_ref[d, r : r + 256, :], b)

        return carry

    lax.fori_loop(0, 8, one, 0)


BLOCK = jax.ShapeDtypeStruct((1024, 512), F32)


def block_product(across, down, far):
    ids = range(8) if far else [0, 1, 3, 4, 5, 7]
    n = len(ids)

    def body(*refs):
        a, b = [None] * 8, [None] * 8
        for at, i in enumerate(ids):
            a[i], b[i] = refs[at], refs[n + at]
        block_kernel(far, a, b, refs[2 * n : 2 * n + 2], *refs[2 * n + 2 :])

    return pl.pallas_call(
        body,
        out_shape=(BLOCK, BLOCK),
        in_specs=[pl.BlockSpec(memory_space=pl.ANY)] * (2 * n),
        scratch_shapes=[
            pltpu.VMEM((8, 1024, 512), BF16),
            pltpu.VMEM((8, 1024, 512), BF16),
            pltpu.SemaphoreType.DMA((2, 8)),
        ],
        compiler_params=KERNEL_PARAMS,
        cost_estimate=pl.CostEstimate(flops=4_300_000_000, transcendentals=0, bytes_accessed=14_000_000),
        name="block_far" if far else "block_near",
    )(*[across[i] for i in ids], *[down[i] for i in ids])


def swap(x, axis):
    return lax.ppermute(x, axis, [(0, 1), (1, 0)])


def shift(x, axis, by):
    n = lax.axis_size(axis)
    return lax.ppermute(x, axis, [(i, (i + by) % n) for i in range(n)])


def send(x, axis, src, dst):
    return lax.ppermute(x, axis, [(src, dst)])


def after(x, *others):
    return lax.optimization_barrier((x, *others))[0]


def gather2(x, axis):
    other = swap(x, axis)
    first = lax.axis_index(axis) == 0
    return jnp.stack([jnp.where(first, x, other), jnp.where(first, other, x)])


def ring4(x, axis):
    return [x, shift(x, axis, -1), shift(x, axis, 2), shift(x, axis, 1)]


def in_order(parts, axis):
    turn = (4 - lax.axis_index(axis)) % 4
    twice = jnp.concatenate(parts + parts[:3])
    size = parts[0].shape[0]
    return lax.dynamic_slice_in_dim(twice, turn * size, 4 * size)


def scatter2(x, axis):
    me = lax.axis_index(axis)
    other = swap(lax.dynamic_index_in_dim(x, 1 - me, 0, False), axis)
    return lax.dynamic_index_in_dim(x, me, 0, False) + other


def scatter4(x, axis):
    me = lax.axis_index(axis)
    pick = lambda ahead: lax.dynamic_index_in_dim(x, (me + ahead) % 4, 0, False)
    return (pick(0) + shift(pick(2), axis, 2)) + (shift(pick(1), axis, 1) + shift(pick(3), axis, -1))


def first_of_pair(x):
    return jnp.where(lax.axis_index("xl") == 0, x, send(x, "xl", 0, 1))


def first_of_ring(x):
    return lax.select_n(lax.axis_index("z"), x, send(x, "z", 0, 1), send(x, "z", 0, 2), send(x, "z", 0, 3))


def transpose_chips(x):
    pairs = []
    for d in range(math.prod(SIZES)):
        k, c, r = d % 2, (d // 2) % 8, d // 16
        pairs.append((d, (c * 8 + r) * 2 + k))
    return lax.ppermute(x, AXES, pairs)


def sum_rows(x):
    x = x + swap(x, "xl")
    x = x + lax.ppermute(x, "z", [(i, i ^ 1) for i in range(4)])
    return x + lax.ppermute(x, "z", [(i, i ^ 2) for i in range(4)])


def embed(occupations, table):
    onehot = jnp.concatenate([(occupations == v).astype(F32) for v in range(3)], axis=1)
    embedded = jnp.dot(onehot, table, precision=lax.Precision.HIGH, preferred_element_type=F32)
    return embedded * lax.rsqrt(jnp.mean(embedded * embedded, axis=-1, keepdims=True) + norm_eps)


def log_derivatives(embedded, weights, biases, heads):
    blocks = []
    for p in range(2):
        hidden = jnp.dot(embedded, weights[p], precision=lax.Precision.HIGH, preferred_element_type=F32)
        blocks.append(heads[p] * jax.nn.sigmoid(hidden + biases[p]))
    return jnp.concatenate(blocks, axis=1)


def outer(a, b):
    return lax.dot_general(a, b, (((1,), (1,)), ((), ())), preferred_element_type=F32)


def outer3(a, b):
    return lax.dot_general(
        a, b, (((1,), (1,)), ((), ())), precision=lax.Precision.HIGH, preferred_element_type=F32
    )


def on_device(occupations, table, weights, biases, heads, energies):
    rows = occupations.shape[0]
    total = rows * 8
    cols = total // 16
    z, xl, xh, y, core = [lax.axis_index(a) for a in AXES]
    row, chip_col = z * 2 + xl, xh * 4 + y
    par = weights.shape[0] * weights.shape[2]

    pair_occ = first_of_pair(occupations.astype(BF16))
    embedded = after(embed(occupations, table), pair_occ)
    first_occ = first_of_ring(pair_occ)
    derivs = log_derivatives(embedded, weights, biases, heads)
    sums = jnp.sum(derivs, axis=0, keepdims=True)
    first_embedded = embed(after(first_occ, sums), table)
    first_derivs = log_derivatives(first_embedded, weights, biases, heads)
    mean = sum_rows(sums) / total
    center = lambda d: ((d - mean) * (1.0 / math.sqrt(total))).astype(BF16)
    own, first = center(derivs), center(first_derivs)

    eye = lambda r, c, r0, c0: jnp.where(
        (lax.broadcasted_iota(jnp.int32, (r, c), 0) + r0) == (lax.broadcasted_iota(jnp.int32, (r, c), 1) + c0),
        diag_shift,
        0.0,
    ).astype(F32)

    pick = first.reshape(2, 4, 4, 2, 16, par)
    pick = lax.dynamic_index_in_dim(lax.dynamic_index_in_dim(pick, z, 1, False), xl, 2, False)
    slab = outer(pick.reshape(128, par), first).reshape(2, 4, 2, 8, rows)
    own_x = after(own, slab)
    turned = transpose_chips(own_x)
    slab = scatter2(slab, "k")
    panel = outer(own_x, first).reshape(2, 4, 2, rows // 16, rows)
    panel = scatter2(panel, "k")
    slab = scatter4(slab, "y")
    own_y = after(own, turned)
    own_next, own_prev = shift(own_y, "y", -1), shift(own_y, "y", 1)
    turned_next, turned_prev = shift(turned, "z", -1), shift(turned, "z", 1)
    slab = scatter2(slab, "xh")
    slab = gather2(gather2(slab, "xh"), "xl")
    beside = swap(after(own, slab), "xh")
    turned_side = swap(after(turned, slab), "xl")
    slab = in_order(ring4(slab.reshape(32, rows), "y"), "y")
    panel = scatter4(after(panel, slab), "y")
    parts = ring4(slab, "z")
    parts = parts + [swap(p, "k") for p in parts]
    own_far = shift(after(own_prev, slab), "y", 1)
    turned_far = shift(after(turned_prev, slab), "z", 1)
    turned_side, beside, *parts = lax.optimization_barrier((turned_side, beside, *parts))
    side_next, side_prev = shift(beside, "y", -1), shift(beside, "y", 1)
    tside_next, tside_prev = (shift(turned_side, "z", -1), shift(turned_side, "z", 1))
    panel = scatter2(after(panel, *parts), "xh")

    low, rest = start_inverse(parts)
    panel, side_next, tside_next, rest = lax.optimization_barrier((panel, side_next, tside_next, rest))
    mine = gather2(panel, "xh").reshape(rows // 8, rows)
    panel_turned = transpose_chips(panel)
    side_far = shift(side_next, "y", -1)
    tside_far = shift(tside_next, "z", -1)

    mid, rest = go_on_inverse(rest, 256)
    panel_turned, mine, rest = lax.optimization_barrier((panel_turned, mine, rest))
    mine = ring4(mine, "y")
    other = gather2(panel_turned, "xl").reshape(rows // 8, rows)

    (high,) = go_on_inverse(rest, 256)
    other, high = lax.optimization_barrier((other, high))
    other = ring4(other, "z")
    first_side = first_of_ring(first_of_pair(after(energies.reshape(8, -1), rest))).reshape(1, -1)

    across = [own, own_next, own_far, own_prev, beside, side_next, side_far, side_prev]
    down = [turned, turned_next, turned_far, turned_prev, turned_side, tside_next, tside_far, tside_prev]
    theirs, block = block_product(across, down, False)
    block = block + swap(theirs, "k")

    mine = gather2(in_order(mine, "y"), "k").reshape(rows, rows)
    other = in_order(other, "z").reshape(2, 4, rows // 16, rows).transpose(1, 0, 2, 3).reshape(cols, rows)
    mine = mine + eye(rows, rows, row * rows, 0)
    other = other + eye(cols, rows, chip_col * rows + core * cols, 0)
    inverse = [low[:, :512], mid[:, :768], high]
    left = jnp.concatenate([outer3(mine[:, : w.shape[1]], w) for w in inverse], 1)
    right = jnp.concatenate([outer3(other[:, : w.shape[1]], w) for w in inverse], 1)
    exact = lambda a, b: lax.dot_general(
        a, b, (((1,), (1,)), ((), ())), precision=lax.Precision.HIGHEST, preferred_element_type=F32
    )
    solved = jnp.concatenate([exact(first_side[:, : w.shape[1]], w) for w in inverse], 1)
    side = energies - jnp.sum(left * solved, axis=1)
    side = jnp.where(row == 0, solved[0], side)
    block = (block + eye(rows, cols, row * rows, chip_col * rows + core * cols)) - outer3(left, right)

    theirs, last = block_product(across, down, True)
    schur = (block + last) + swap(theirs, "k")
    return schur, side


def solution(mesh):
    torus = Mesh(mesh.devices.reshape(SIZES), AXES)
    placed = (P(ROW, None), P(), P(None, None, COL), P(None, COL), P(None, COL), P(ROW))


    return jax.shard_map(on_device, mesh=torus, in_specs=placed, out_specs=(P(ROW, COL), P(ROW)), check_vma=False)
```

```python
import math

import jax
import jax.numpy as jnp
from jax import lax
from jax.experimental import pallas as pl
from jax.experimental.pallas import tpu as pltpu
from jax.sharding import Mesh
from jax.sharding import PartitionSpec as P

AXES = ("z", "xl", "xh", "y", "k")
SIZES = (4, 2, 2, 4, 2)
ROW = ("z", "xl")
COL = ("xh", "y", "k")
F32 = jnp.float32
BF16 = jnp.bfloat16


norm_eps = 1e-06
diag_shift = 0.05

NB = 128
PG = 16


def halves(x):
    hi = x.astype(BF16)
    return hi, (x - hi.astype(F32)).astype(BF16)


def dot3(a, b, dims=((1,), (0,))):
    (ah, al), (bh, bl) = a, b
    d = lambda u, v: lax.dot_general(u, v, (dims, ((), ())), preferred_element_type=F32)
    return d(ah, bh) + (d(ah, bl) + d(al, bh))


def factor_block(x_ref, f_ref, gh_ref, gl_ref):
    row = lax.broadcasted_iota(jnp.int32, (PG, NB), 0)
    lane = lax.broadcasted_iota(jnp.int32, (NB, NB), 1)
    for g in range(NB // PG):
        lo = g * PG
        p0 = x_ref[lo : lo + PG, :NB]
        p1 = x_ref[lo : lo + PG, NB:]
        cols = [jnp.broadcast_to(p0[:, lo + j : lo + j + 1], (PG, NB)) for j in range(PG)]
        f1 = jnp.zeros_like(p1)
        for i in range(PG):
            up = lambda v: jnp.broadcast_to(v[i : i + 1, :], (PG, NB))
            piv = up(cols[i])
            inv = 1.0 / piv
            here = row == i
            a1 = up(p1)
            f1 = jnp.where(here, a1 * lax.rsqrt(piv), f1)
            a0 = up(p0) * inv
            a1 = a1 * inv
            ci = cols[i]
            for j in range(i + 1, PG):
                b = up(cols[j]) * inv
                cols[j] = jnp.where(here, b, cols[j] - ci * b)
            p0 = jnp.where(here, a0, p0 - ci * a0)
            p1 = jnp.where(here, a1, p1 - ci * a1)
        f_ref[lo : lo + PG, :] = f1
        if g + 1 < NB // PG:
            for half, v in ((slice(0, NB), p0), (slice(NB, 2 * NB), p1)):
                gh_ref[lo : lo + PG, half], gl_ref[lo : lo + PG, half] = halves(v)
            rest = slice(lo + PG, NB)
            n = NB - lo - PG
            inside = (lane[:n] >= lo) & (lane[:n] < lo + PG)
            left = halves(jnp.where(inside, x_ref[rest, :NB], 0.0))
            x_ref[rest, :] = x_ref[rest, :] - dot3(left, (gh_ref[...], gl_ref[...]))


def eliminate(t_ref, w_ref, first, x_ref, f_ref, gh_ref, gl_ref, yh_ref, yl_ref):
    n = t_ref.shape[1]
    gh_ref[...] = jnp.zeros_like(gh_ref)
    gl_ref[...] = jnp.zeros_like(gl_ref)
    eye = lax.broadcasted_iota(jnp.int32, (NB, NB), 0) == lax.broadcasted_iota(jnp.int32, (NB, NB), 1)
    ident = eye.astype(F32)
    wide = lax.broadcasted_iota(jnp.int32, (NB, n), 1)

    def step(b, carry):
        at = pl.multiple_of(first + b * NB, NB)
        mine = pl.ds(pl.multiple_of(b * NB, NB), NB)
        here = pl.ds(at, NB)
        x_ref[:, :NB] = t_ref[mine, here] + diag_shift * ident
        x_ref[:, NB:] = ident
        factor_block(x_ref, f_ref, gh_ref, gl_ref)
        linv = halves(f_ref[...])
        t_ref[mine, here] = ident
        y = dot3(linv, halves(t_ref[mine, :]))
        w_ref[mine, :] = jnp.where(wide < at + NB, y, 0.0)
        yh_ref[...], yl_ref[...] = halves(y)

        def below(r, c):
            rows = pl.ds(pl.multiple_of(r * NB, NB), NB)
            mult = dot3(halves(t_ref[rows, here]), linv, ((1,), (1,)))
            t_ref[rows, here] = jnp.zeros((NB, NB), F32)
            t_ref[rows, :] = t_ref[rows, :] - dot3(halves(mult), (yh_ref[...], yl_ref[...]))
            return c

        lax.fori_loop(b + 1, t_ref.shape[0] // NB, below, 0)
        return carry

    lax.fori_loop(0, w_ref.shape[0] // NB, step, 0)


def first_half(*refs):
    parts, (w_ref, out_ref, t_ref, *scratch, sems) = refs[:8], refs[8:]
    z, k = lax.axis_index("z"), lax.axis_index("k")
    copies = []
    for dk in range(2):
        for dz in range(4):
            i = dk * 4 + dz
            at = ((k + dk) % 2) * 512 + ((z + dz) % 4) * 128
            copies.append(pltpu.make_async_copy(parts[i], t_ref.at[pl.ds(pl.multiple_of(at, 128), 128)], sems.at[i]))
    for c in copies:
        c.start()
    for c in copies:
        c.wait()
    eliminate(t_ref, w_ref, 0, *scratch)
    out_ref[...] = t_ref[512:, :]


def later_part(first, a_ref, w_ref, *refs):
    done = w_ref.shape[0]
    (out_ref,), (t_ref, *scratch) = (refs[:1], refs[1:]) if first + done < 1024 else ((None,), refs)
    t_ref[...] = a_ref[...]
    eliminate(t_ref, w_ref, first, *scratch)
    if out_ref is not None:
        out_ref[...] = t_ref[done:, :]


FACTOR_SCRATCH = [
    pltpu.VMEM((NB, 2 * NB), F32),
    pltpu.VMEM((NB, NB), F32),
    pltpu.VMEM((NB, 2 * NB), BF16),
    pltpu.VMEM((NB, 2 * NB), BF16),
    pltpu.VMEM((NB, 1024), BF16),
    pltpu.VMEM((NB, 1024), BF16),
]
KERNEL_PARAMS = pltpu.CompilerParams(vmem_limit_bytes=40 * 1024 * 1024)


def factor_cost(flops):
    return pl.CostEstimate(flops=flops, transcendentals=0, bytes_accessed=8_000_000)


def lines(n):
    return jax.ShapeDtypeStruct((n, 1024), F32)


def start_inverse(parts):
    return pl.pallas_call(
        first_half,
        out_shape=(lines(512), lines(512)),
        in_specs=[pl.BlockSpec(memory_space=pl.ANY)] * 8,
        scratch_shapes=[pltpu.VMEM((1024, 1024), F32), *FACTOR_SCRATCH, pltpu.SemaphoreType.DMA((8,))],
        compiler_params=KERNEL_PARAMS,
        cost_estimate=factor_cost(15_000_000_000),
        name="inverse_first",
    )(*parts)


def go_on_inverse(rest, count):
    left = rest.shape[0]
    return pl.pallas_call(
        lambda *refs: later_part(1024 - left, *refs),
        out_shape=(lines(count), lines(left - count)) if left > count else (lines(count),),
        scratch_shapes=[pltpu.VMEM((left, 1024), F32), *FACTOR_SCRATCH],
        compiler_params=KERNEL_PARAMS,
        cost_estimate=factor_cost(5_000_000_000),
    )(rest)


def block_kernel(far, across, down, outs, a_ref, b_ref, sems):
    z, xl, xh, y, k = [lax.axis_index(a) for a in AXES]
    wanted = lambda d: ((d % 4 == (y + 2) % 4) | (d // 2 == (z + 2) % 4)) == far
    copies = []
    for i in range(8):
        step, flip = i % 4, i // 4
        if across[i] is not None:
            d = ((xh + flip) % 2) * 4 + (y + step) % 4
            copies.append((d, pltpu.make_async_copy(across[i], a_ref.at[d], sems.at[0, i])))
            d = ((z + step) % 4) * 2 + (xl + flip) % 2
            copies.append((d, pltpu.make_async_copy(down[i], b_ref.at[d], sems.at[1, i])))
    for d, c in copies:
        pl.when(wanted(d))(c.start)
    for out in outs:
        out[...] = jnp.zeros_like(out)
    for d, c in copies:
        pl.when(wanted(d))(c.wait)

    def one(d, carry):
        @pl.when(wanted(d))
        def _():
            for theirs, out in zip((1, 0), outs):
                b = b_ref[d, pl.ds(pl.multiple_of(((k + theirs) % 2) * 512, 512), 512), :]
                for r in range(0, 1024, 256):
                    out[r : r + 256, :] += outer(a_ref[d, r : r + 256, :], b)

        return carry

    lax.fori_loop(0, 8, one, 0)


BLOCK = jax.ShapeDtypeStruct((1024, 512), F32)


def block_product(across, down, far):
    ids = range(8) if far else [0, 1, 3, 4, 5, 7]
    n = len(ids)

    def body(*refs):
        a, b = [None] * 8, [None] * 8
        for at, i in enumerate(ids):
            a[i], b[i] = refs[at], refs[n + at]
        block_kernel(far, a, b, refs[2 * n : 2 * n + 2], *refs[2 * n + 2 :])

    return pl.pallas_call(
        body,
        out_shape=(BLOCK, BLOCK),
        in_specs=[pl.BlockSpec(memory_space=pl.ANY)] * (2 * n),
        scratch_shapes=[
            pltpu.VMEM((8, 1024, 512), BF16),
            pltpu.VMEM((8, 1024, 512), BF16),
            pltpu.SemaphoreType.DMA((2, 8)),
        ],
        compiler_params=KERNEL_PARAMS,
        cost_estimate=pl.CostEstimate(flops=4_300_000_000, transcendentals=0, bytes_accessed=14_000_000),
        name="block_far" if far else "block_near",
    )(*[across[i] for i in ids], *[down[i] for i in ids])


def swap(x, axis):
    return lax.ppermute(x, axis, [(0, 1), (1, 0)])


def shift(x, axis, by):
    n = lax.axis_size(axis)
    return lax.ppermute(x, axis, [(i, (i + by) % n) for i in range(n)])


def send(x, axis, src, dst):
    return lax.ppermute(x, axis, [(src, dst)])


def after(x, *others):
    return lax.optimization_barrier((x, *others))[0]


def gather2(x, axis):
    other = swap(x, axis)
    first = lax.axis_index(axis) == 0
    return jnp.stack([jnp.where(first, x, other), jnp.where(first, other, x)])


def ring4(x, axis):
    return [x, shift(x, axis, -1), shift(x, axis, 2), shift(x, axis, 1)]


def in_order(parts, axis):
    size = parts[0].shape[0]
    out = jnp.zeros((4 * size,) + parts[0].shape[1:], parts[0].dtype)
    for step, part in enumerate(parts):
        at = (lax.axis_index(axis) + step) % 4
        out = lax.dynamic_update_slice_in_dim(out, part, at * size, 0)
    return out


def scatter2(x, axis):
    me = lax.axis_index(axis)
    other = swap(lax.dynamic_index_in_dim(x, 1 - me, 0, False), axis)
    return lax.dynamic_index_in_dim(x, me, 0, False) + other


def scatter4(x, axis):
    me = lax.axis_index(axis)
    pick = lambda ahead: lax.dynamic_index_in_dim(x, (me + ahead) % 4, 0, False)
    return (pick(0) + shift(pick(2), axis, 2)) + (shift(pick(1), axis, 1) + shift(pick(3), axis, -1))


def first_of_pair(x):
    return jnp.where(lax.axis_index("xl") == 0, x, send(x, "xl", 0, 1))


def first_of_ring(x):
    return lax.select_n(lax.axis_index("z"), x, send(x, "z", 0, 1), send(x, "z", 0, 2), send(x, "z", 0, 3))


def transpose_chips(x):
    pairs = []
    for d in range(math.prod(SIZES)):
        k, c, r = d % 2, (d // 2) % 8, d // 16
        pairs.append((d, (c * 8 + r) * 2 + k))
    return lax.ppermute(x, AXES, pairs)


def sum_rows(x):
    x = x + swap(x, "xl")
    x = x + lax.ppermute(x, "z", [(i, i ^ 1) for i in range(4)])
    return x + lax.ppermute(x, "z", [(i, i ^ 2) for i in range(4)])


def embed(occupations, table):
    onehot = jnp.concatenate([(occupations == v).astype(F32) for v in range(3)], axis=1)
    embedded = jnp.dot(onehot, table, precision=lax.Precision.HIGH, preferred_element_type=F32)
    return embedded * lax.rsqrt(jnp.mean(embedded * embedded, axis=-1, keepdims=True) + norm_eps)


def log_derivatives(embedded, weights, biases, heads):
    blocks = []
    for p in range(2):
        hidden = jnp.dot(embedded, weights[p], precision=lax.Precision.HIGH, preferred_element_type=F32)
        blocks.append(heads[p] * jax.nn.sigmoid(hidden + biases[p]))
    return jnp.concatenate(blocks, axis=1)


def outer(a, b):
    return lax.dot_general(a, b, (((1,), (1,)), ((), ())), preferred_element_type=F32)


def outer3(a, b):
    return lax.dot_general(
        a, b, (((1,), (1,)), ((), ())), precision=lax.Precision.HIGH, preferred_element_type=F32
    )


def on_device(occupations, table, weights, biases, heads, energies):
    rows = occupations.shape[0]
    total = rows * 8
    cols = total // 16
    z, xl, xh, y, core = [lax.axis_index(a) for a in AXES]
    row, chip_col = z * 2 + xl, xh * 4 + y
    par = weights.shape[0] * weights.shape[2]

    side_parts, remains = [], energies.reshape(-1, occupations.shape[1])
    for _ in range(3):
        rounded = lax.reduce_precision(remains, 8, 7)
        side_parts.append(rounded.astype(BF16))
        remains = remains - rounded
    pair_occ = first_of_pair(jnp.concatenate([occupations.astype(BF16), *side_parts]))
    embedded = embed(occupations, table)
    first_occ = after(first_of_ring(pair_occ), embedded)
    first_side = jnp.sum(first_occ[rows:].astype(F32).reshape(3, rows), axis=0, keepdims=True)
    first_occ = first_occ[:rows]
    derivs = log_derivatives(embedded, weights, biases, heads)
    sums = jnp.sum(derivs, axis=0, keepdims=True)
    first_embedded = embed(after(first_occ, sums), table)
    first_derivs = log_derivatives(first_embedded, weights, biases, heads)
    mean = sum_rows(sums) / total
    center = lambda d: ((d - mean) * (1.0 / math.sqrt(total))).astype(BF16)
    own, first = center(derivs), center(first_derivs)

    eye = lambda r, c, r0, c0: jnp.where(
        (lax.broadcasted_iota(jnp.int32, (r, c), 0) + r0) == (lax.broadcasted_iota(jnp.int32, (r, c), 1) + c0),
        diag_shift,
        0.0,
    ).astype(F32)

    pick = first.reshape(2, 4, 4, 2, 16, par)
    pick = lax.dynamic_index_in_dim(lax.dynamic_index_in_dim(pick, z, 1, False), xl, 2, False)
    slab = outer(pick.reshape(128, par), first).reshape(2, 4, 2, 8, rows)
    slab = scatter2(slab, "k")
    panel = outer(after(own, slab), first).reshape(2, 4, 2, rows // 16, rows)
    slab = scatter4(slab, "y")
    panel = scatter2(panel, "k")
    slab = scatter2(slab, "xh")
    slab = gather2(gather2(slab, "xh"), "xl")
    slab = in_order(ring4(slab.reshape(32, rows), "y"), "y")
    parts = ring4(slab, "z")
    parts = parts + [swap(p, "k") for p in parts]
    own_y = after(own, slab)
    turned = transpose_chips(own_y)
    beside = swap(own_y, "xh")
    panel = scatter4(after(panel, slab), "y")
    own_next, own_prev = shift(own_y, "y", -1), shift(own_y, "y", 1)
    beside, panel, *parts = lax.optimization_barrier((beside, panel, *parts))
    side_next, side_prev = shift(beside, "y", -1), shift(beside, "y", 1)
    panel = scatter2(panel, "xh")

    low, rest = start_inverse(parts)
    panel, turned, own_prev, rest = lax.optimization_barrier((panel, turned, own_prev, rest))
    turned_next, turned_prev = shift(turned, "z", -1), shift(turned, "z", 1)
    turned_side = swap(turned, "xl")
    mine = gather2(panel, "xh").reshape(rows // 8, rows)
    panel_turned = transpose_chips(panel)
    own_far = shift(own_prev, "y", 1)

    mid, rest = go_on_inverse(rest, 256)
    panel_turned, mine, side_next, rest = lax.optimization_barrier((panel_turned, mine, side_next, rest))
    mine = ring4(mine, "y")
    other = gather2(panel_turned, "xl").reshape(rows // 8, rows)
    side_far = shift(side_next, "y", -1)

    (high,) = go_on_inverse(rest, 256)
    other, turned_side, turned_prev, high = lax.optimization_barrier((other, turned_side, turned_prev, high))
    tside_next, tside_prev = (shift(turned_side, "z", -1), shift(turned_side, "z", 1))
    other = ring4(other, "z")
    turned_far = shift(turned_prev, "z", 1)
    tside_far = shift(tside_next, "z", -1)

    across = [own, own_next, own_far, own_prev, beside, side_next, side_far, side_prev]
    down = [turned, turned_next, turned_far, turned_prev, turned_side, tside_next, tside_far, tside_prev]
    theirs, block = block_product(across, down, False)
    block = block + swap(theirs, "k")

    mine = gather2(in_order(mine, "y"), "k").reshape(rows, rows)
    other = in_order(other, "z").reshape(2, 4, rows // 16, rows).transpose(1, 0, 2, 3).reshape(cols, rows)
    mine = mine + eye(rows, rows, row * rows, 0)
    other = other + eye(cols, rows, chip_col * rows + core * cols, 0)
    inverse = [low[:, :512], mid[:, :768], high]
    left = jnp.concatenate([outer3(mine[:, : w.shape[1]], w) for w in inverse], 1)
    right = jnp.concatenate([outer3(other[:, : w.shape[1]], w) for w in inverse], 1)
    exact = lambda a, b: lax.dot_general(
        a, b, (((1,), (1,)), ((), ())), precision=lax.Precision.HIGHEST, preferred_element_type=F32
    )
    solved = jnp.concatenate([exact(first_side[:, : w.shape[1]], w) for w in inverse], 1)
    side = energies - jnp.sum(left * solved, axis=1)
    side = jnp.where(row == 0, solved[0], side)
    block = (block + eye(rows, cols, row * rows, chip_col * rows + core * cols)) - outer3(left, right)

    down[6], block = lax.optimization_barrier((tside_far, block))
    theirs, last = block_product(across, down, True)
    schur = (block + last) + swap(theirs, "k")
    return schur, side


def solution(mesh):
    torus = Mesh(mesh.devices.reshape(SIZES), AXES)
    placed = (P(ROW, None), P(), P(None, None, COL), P(None, COL), P(None, COL), P(ROW))


    return jax.shard_map(on_device, mesh=torus, in_specs=placed, out_specs=(P(ROW, COL), P(ROW)), check_vma=False)
```

```python
import math

import jax
import jax.numpy as jnp
from jax import lax
from jax.experimental import pallas as pl
from jax.experimental.pallas import tpu as pltpu
from jax.sharding import Mesh
from jax.sharding import PartitionSpec as P

AXES = ("z", "xl", "xh", "y", "k")
SIZES = (4, 2, 2, 4, 2)
ROW = ("z", "xl")
COL = ("xh", "y", "k")
F32 = jnp.float32
BF16 = jnp.bfloat16


norm_eps = 1e-06
diag_shift = 0.05

NB = 128
PG = 16


def halves(x):
    hi = x.astype(BF16)
    return hi, (x - hi.astype(F32)).astype(BF16)


def dot3(a, b, dims=((1,), (0,))):
    (ah, al), (bh, bl) = a, b
    d = lambda u, v: lax.dot_general(u, v, (dims, ((), ())), preferred_element_type=F32)
    return d(ah, bh) + (d(ah, bl) + d(al, bh))


def factor_block(x_ref, f_ref, gh_ref, gl_ref):
    row = lax.broadcasted_iota(jnp.int32, (PG, NB), 0)
    lane = lax.broadcasted_iota(jnp.int32, (NB, NB), 1)
    for g in range(NB // PG):
        lo = g * PG
        p0 = x_ref[lo : lo + PG, :NB]
        p1 = x_ref[lo : lo + PG, NB:]
        cols = [jnp.broadcast_to(p0[:, lo + j : lo + j + 1], (PG, NB)) for j in range(PG)]
        f1 = jnp.zeros_like(p1)
        for i in range(PG):
            up = lambda v: jnp.broadcast_to(v[i : i + 1, :], (PG, NB))
            piv = up(cols[i])
            inv = 1.0 / piv
            here = row == i
            a1 = up(p1)
            f1 = jnp.where(here, a1 * lax.rsqrt(piv), f1)
            a0 = up(p0) * inv
            a1 = a1 * inv
            ci = cols[i]
            for j in range(i + 1, PG):
                b = up(cols[j]) * inv
                cols[j] = jnp.where(here, b, cols[j] - ci * b)
            p0 = jnp.where(here, a0, p0 - ci * a0)
            p1 = jnp.where(here, a1, p1 - ci * a1)
        f_ref[lo : lo + PG, :] = f1
        if g + 1 < NB // PG:
            for half, v in ((slice(0, NB), p0), (slice(NB, 2 * NB), p1)):
                gh_ref[lo : lo + PG, half], gl_ref[lo : lo + PG, half] = halves(v)
            rest = slice(lo + PG, NB)
            n = NB - lo - PG
            inside = (lane[:n] >= lo) & (lane[:n] < lo + PG)
            left = halves(jnp.where(inside, x_ref[rest, :NB], 0.0))
            x_ref[rest, :] = x_ref[rest, :] - dot3(left, (gh_ref[...], gl_ref[...]))


def eliminate(t_ref, w_ref, first, x_ref, f_ref, gh_ref, gl_ref, yh_ref, yl_ref):
    n = t_ref.shape[1]
    gh_ref[...] = jnp.zeros_like(gh_ref)
    gl_ref[...] = jnp.zeros_like(gl_ref)
    eye = lax.broadcasted_iota(jnp.int32, (NB, NB), 0) == lax.broadcasted_iota(jnp.int32, (NB, NB), 1)
    ident = eye.astype(F32)
    wide = lax.broadcasted_iota(jnp.int32, (NB, n), 1)

    def step(b, carry):
        at = pl.multiple_of(first + b * NB, NB)
        mine = pl.ds(pl.multiple_of(b * NB, NB), NB)
        here = pl.ds(at, NB)
        x_ref[:, :NB] = t_ref[mine, here] + diag_shift * ident
        x_ref[:, NB:] = ident
        factor_block(x_ref, f_ref, gh_ref, gl_ref)
        linv = halves(f_ref[...])
        t_ref[mine, here] = ident
        y = dot3(linv, halves(t_ref[mine, :]))
        w_ref[mine, :] = jnp.where(wide < at + NB, y, 0.0)
        yh_ref[...], yl_ref[...] = halves(y)

        def below(r, c):
            rows = pl.ds(pl.multiple_of(r * NB, NB), NB)
            mult = dot3(halves(t_ref[rows, here]), linv, ((1,), (1,)))
            t_ref[rows, here] = jnp.zeros((NB, NB), F32)
            t_ref[rows, :] = t_ref[rows, :] - dot3(halves(mult), (yh_ref[...], yl_ref[...]))
            return c

        lax.fori_loop(b + 1, t_ref.shape[0] // NB, below, 0)
        return carry

    lax.fori_loop(0, w_ref.shape[0] // NB, step, 0)


def first_half(*refs):
    parts, (w_ref, out_ref, t_ref, *scratch, sems) = refs[:8], refs[8:]
    z, k = lax.axis_index("z"), lax.axis_index("k")
    copies = []
    for dk in range(2):
        for dz in range(4):
            i = dk * 4 + dz
            at = ((k + dk) % 2) * 512 + ((z + dz) % 4) * 128
            copies.append(pltpu.make_async_copy(parts[i], t_ref.at[pl.ds(pl.multiple_of(at, 128), 128)], sems.at[i]))
    for c in copies:
        c.start()
    for c in copies:
        c.wait()
    eliminate(t_ref, w_ref, 0, *scratch)
    out_ref[...] = t_ref[512:, :]


def later_part(first, a_ref, w_ref, *refs):
    done = w_ref.shape[0]
    (out_ref,), (t_ref, *scratch) = (refs[:1], refs[1:]) if first + done < 1024 else ((None,), refs)
    t_ref[...] = a_ref[...]
    eliminate(t_ref, w_ref, first, *scratch)
    if out_ref is not None:
        out_ref[...] = t_ref[done:, :]


FACTOR_SCRATCH = [
    pltpu.VMEM((NB, 2 * NB), F32),
    pltpu.VMEM((NB, NB), F32),
    pltpu.VMEM((NB, 2 * NB), BF16),
    pltpu.VMEM((NB, 2 * NB), BF16),
    pltpu.VMEM((NB, 1024), BF16),
    pltpu.VMEM((NB, 1024), BF16),
]
KERNEL_PARAMS = pltpu.CompilerParams(vmem_limit_bytes=40 * 1024 * 1024)


def factor_cost(flops):
    return pl.CostEstimate(flops=flops, transcendentals=0, bytes_accessed=8_000_000)


def lines(n):
    return jax.ShapeDtypeStruct((n, 1024), F32)


def start_inverse(parts):
    return pl.pallas_call(
        first_half,
        out_shape=(lines(512), lines(512)),
        in_specs=[pl.BlockSpec(memory_space=pl.ANY)] * 8,
        scratch_shapes=[pltpu.VMEM((1024, 1024), F32), *FACTOR_SCRATCH, pltpu.SemaphoreType.DMA((8,))],
        compiler_params=KERNEL_PARAMS,
        cost_estimate=factor_cost(15_000_000_000),
        name="inverse_first",
    )(*parts)


def go_on_inverse(rest, count):
    left = rest.shape[0]
    return pl.pallas_call(
        lambda *refs: later_part(1024 - left, *refs),
        out_shape=(lines(count), lines(left - count)) if left > count else (lines(count),),
        scratch_shapes=[pltpu.VMEM((left, 1024), F32), *FACTOR_SCRATCH],
        compiler_params=KERNEL_PARAMS,
        cost_estimate=factor_cost(5_000_000_000),
    )(rest)


def block_kernel(far, across, down, outs, a_ref, b_ref, sems):
    z, xl, xh, y, k = [lax.axis_index(a) for a in AXES]
    wanted = lambda d: ((d % 4 == (y + 2) % 4) | (d // 2 == (z + 2) % 4)) == far
    copies = []
    for i in range(8):
        step, flip = i % 4, i // 4
        if across[i] is not None:
            d = ((xh + flip) % 2) * 4 + (y + step) % 4
            copies.append((d, pltpu.make_async_copy(across[i], a_ref.at[d], sems.at[0, i])))
            d = ((z + step) % 4) * 2 + (xl + flip) % 2
            copies.append((d, pltpu.make_async_copy(down[i], b_ref.at[d], sems.at[1, i])))
    for d, c in copies:
        pl.when(wanted(d))(c.start)
    for out in outs:
        out[...] = jnp.zeros_like(out)
    for d, c in copies:
        pl.when(wanted(d))(c.wait)

    def one(d, carry):
        @pl.when(wanted(d))
        def _():
            for theirs, out in zip((1, 0), outs):
                b = b_ref[d, pl.ds(pl.multiple_of(((k + theirs) % 2) * 512, 512), 512), :]
                for r in range(0, 1024, 256):
                    out[r : r + 256, :] += outer(a_ref[d, r : r + 256, :], b)

        return carry

    lax.fori_loop(0, 8, one, 0)


BLOCK = jax.ShapeDtypeStruct((1024, 512), F32)


def block_product(across, down, far):
    ids = range(8) if far else [0, 1, 3, 4, 5, 7]
    n = len(ids)

    def body(*refs):
        a, b = [None] * 8, [None] * 8
        for at, i in enumerate(ids):
            a[i], b[i] = refs[at], refs[n + at]
        block_kernel(far, a, b, refs[2 * n : 2 * n + 2], *refs[2 * n + 2 :])

    return pl.pallas_call(
        body,
        out_shape=(BLOCK, BLOCK),
        in_specs=[pl.BlockSpec(memory_space=pl.ANY)] * (2 * n),
        scratch_shapes=[
            pltpu.VMEM((8, 1024, 512), BF16),
            pltpu.VMEM((8, 1024, 512), BF16),
            pltpu.SemaphoreType.DMA((2, 8)),
        ],
        compiler_params=KERNEL_PARAMS,
        cost_estimate=pl.CostEstimate(flops=4_300_000_000, transcendentals=0, bytes_accessed=14_000_000),
        name="block_far" if far else "block_near",
    )(*[across[i] for i in ids], *[down[i] for i in ids])


def swap(x, axis):
    return lax.ppermute(x, axis, [(0, 1), (1, 0)])


def shift(x, axis, by):
    n = lax.axis_size(axis)
    return lax.ppermute(x, axis, [(i, (i + by) % n) for i in range(n)])


def send(x, axis, src, dst):
    return lax.ppermute(x, axis, [(src, dst)])


def after(x, *others):
    return lax.optimization_barrier((x, *others))[0]


def gather2(x, axis):
    other = swap(x, axis)
    first = lax.axis_index(axis) == 0
    return jnp.stack([jnp.where(first, x, other), jnp.where(first, other, x)])


def ring4(x, axis):
    return [x, shift(x, axis, -1), shift(x, axis, 2), shift(x, axis, 1)]


def in_order(parts, axis):
    size = parts[0].shape[0]
    out = jnp.zeros((4 * size,) + parts[0].shape[1:], parts[0].dtype)
    for step, part in enumerate(parts):
        at = (lax.axis_index(axis) + step) % 4
        out = lax.dynamic_update_slice_in_dim(out, part, at * size, 0)
    return out


def scatter2(x, axis):
    me = lax.axis_index(axis)
    other = swap(lax.dynamic_index_in_dim(x, 1 - me, 0, False), axis)
    return lax.dynamic_index_in_dim(x, me, 0, False) + other


def scatter4(x, axis):
    me = lax.axis_index(axis)
    pick = lambda ahead: lax.dynamic_index_in_dim(x, (me + ahead) % 4, 0, False)
    return (pick(0) + shift(pick(2), axis, 2)) + (shift(pick(1), axis, 1) + shift(pick(3), axis, -1))


def first_of_pair(x):
    return jnp.where(lax.axis_index("xl") == 0, x, send(x, "xl", 0, 1))


def first_of_ring(x):
    return lax.select_n(lax.axis_index("z"), x, send(x, "z", 0, 1), send(x, "z", 0, 2), send(x, "z", 0, 3))


def transpose_chips(x):
    pairs = []
    for d in range(math.prod(SIZES)):
        k, c, r = d % 2, (d // 2) % 8, d // 16
        pairs.append((d, (c * 8 + r) * 2 + k))
    return lax.ppermute(x, AXES, pairs)


def sum_rows(x):
    x = x + swap(x, "xl")
    x = x + lax.ppermute(x, "z", [(i, i ^ 1) for i in range(4)])
    return x + lax.ppermute(x, "z", [(i, i ^ 2) for i in range(4)])


def embed(occupations, table):
    onehot = jnp.concatenate([(occupations == v).astype(F32) for v in range(3)], axis=1)
    embedded = jnp.dot(onehot, table, precision=lax.Precision.HIGH, preferred_element_type=F32)
    return embedded * lax.rsqrt(jnp.mean(embedded * embedded, axis=-1, keepdims=True) + norm_eps)


def log_derivatives(embedded, weights, biases, heads):
    blocks = []
    for p in range(2):
        hidden = jnp.dot(embedded, weights[p], precision=lax.Precision.HIGH, preferred_element_type=F32)
        blocks.append(heads[p] * jax.nn.sigmoid(hidden + biases[p]))
    return jnp.concatenate(blocks, axis=1)


def outer(a, b):
    return lax.dot_general(a, b, (((1,), (1,)), ((), ())), preferred_element_type=F32)


def outer3(a, b):
    return lax.dot_general(
        a, b, (((1,), (1,)), ((), ())), precision=lax.Precision.HIGH, preferred_element_type=F32
    )


def on_device(occupations, table, weights, biases, heads, energies):
    rows = occupations.shape[0]
    total = rows * 8
    cols = total // 16
    z, xl, xh, y, core = [lax.axis_index(a) for a in AXES]
    row, chip_col = z * 2 + xl, xh * 4 + y
    par = weights.shape[0] * weights.shape[2]

    side_parts, remains = [], energies.reshape(-1, occupations.shape[1])
    for _ in range(3):
        rounded = lax.reduce_precision(remains, 8, 7)
        side_parts.append(rounded.astype(BF16))
        remains = remains - rounded
    pair_occ = first_of_pair(jnp.concatenate([occupations.astype(BF16), *side_parts]))
    embedded = embed(occupations, table)
    first_occ = after(first_of_ring(pair_occ), embedded)
    first_side = jnp.sum(first_occ[rows:].astype(F32).reshape(3, rows), axis=0, keepdims=True)
    first_occ = first_occ[:rows]
    derivs = log_derivatives(embedded, weights, biases, heads)
    sums = jnp.sum(derivs, axis=0, keepdims=True)
    first_embedded = embed(after(first_occ, sums), table)
    first_derivs = log_derivatives(first_embedded, weights, biases, heads)
    mean = sum_rows(sums) / total
    center = lambda d: ((d - mean) * (1.0 / math.sqrt(total))).astype(BF16)
    own, first = center(derivs), center(first_derivs)

    eye = lambda r, c, r0, c0: jnp.where(
        (lax.broadcasted_iota(jnp.int32, (r, c), 0) + r0) == (lax.broadcasted_iota(jnp.int32, (r, c), 1) + c0),
        diag_shift,
        0.0,
    ).astype(F32)

    pick = first.reshape(2, 4, 4, 2, 16, par)
    pick = lax.dynamic_index_in_dim(lax.dynamic_index_in_dim(pick, z, 1, False), xl, 2, False)
    slab = outer(pick.reshape(128, par), first).reshape(2, 4, 2, 8, rows)
    slab = scatter2(slab, "k")
    panel = outer(after(own, slab), first).reshape(2, 4, 2, rows // 16, rows)
    slab = scatter4(slab, "y")
    panel = scatter2(panel, "k")
    slab = scatter2(slab, "xh")
    panel = scatter4(after(panel, slab), "y")
    slab = gather2(gather2(slab, "xh"), "xl")
    slab = in_order(ring4(slab.reshape(32, rows), "y"), "y")
    parts = ring4(slab, "z")
    parts = parts + [swap(p, "k") for p in parts]
    panel = scatter2(after(panel, slab), "xh")
    mine = gather2(panel, "xh").reshape(rows // 8, rows)
    other = transpose_chips(panel)
    own_y = after(own, panel)
    turned = transpose_chips(own_y)
    beside = swap(own_y, "xh")
    mine = ring4(mine, "y")
    other = gather2(other, "xl").reshape(rows // 8, rows)
    own_next, own_prev = shift(own_y, "y", -1), shift(own_y, "y", 1)

    low, rest = start_inverse(parts)
    other, beside, turned, own_prev, rest = lax.optimization_barrier((other, beside, turned, own_prev, rest))
    other = ring4(other, "z")
    turned_next, turned_prev = shift(turned, "z", -1), shift(turned, "z", 1)
    turned_side = swap(turned, "xl")
    side_next, side_prev = shift(beside, "y", -1), shift(beside, "y", 1)
    own_far = shift(own_prev, "y", 1)
    mid, rest = go_on_inverse(rest, 256)
    (high,) = go_on_inverse(rest, 256)
    turned_side, high = lax.optimization_barrier((turned_side, high))
    tside_next, tside_prev = (shift(turned_side, "z", -1), shift(turned_side, "z", 1))
    turned_far = shift(after(turned_prev, high), "z", 1)
    side_far = shift(after(side_next, high), "y", -1)
    tside_far = shift(tside_next, "z", -1)

    across = [own, own_next, own_far, own_prev, beside, side_next, side_far, side_prev]
    down = [turned, turned_next, turned_far, turned_prev, turned_side, tside_next, tside_far, tside_prev]
    theirs, block = block_product(across, down, False)
    block = block + swap(theirs, "k")

    mine = gather2(in_order(mine, "y"), "k").reshape(rows, rows)
    other = in_order(other, "z").reshape(2, 4, rows // 16, rows).transpose(1, 0, 2, 3).reshape(cols, rows)
    mine = mine + eye(rows, rows, row * rows, 0)
    other = other + eye(cols, rows, chip_col * rows + core * cols, 0)
    inverse = [low[:, :512], mid[:, :768], high]
    left = jnp.concatenate([outer3(mine[:, : w.shape[1]], w) for w in inverse], 1)
    right = jnp.concatenate([outer3(other[:, : w.shape[1]], w) for w in inverse], 1)
    exact = lambda a, b: lax.dot_general(
        a, b, (((1,), (1,)), ((), ())), precision=lax.Precision.HIGHEST, preferred_element_type=F32
    )
    solved = jnp.concatenate([exact(first_side[:, : w.shape[1]], w) for w in inverse], 1)
    side = energies - jnp.sum(left * solved, axis=1)
    side = jnp.where(row == 0, solved[0], side)
    block = (block + eye(rows, cols, row * rows, chip_col * rows + core * cols)) - outer3(left, right)

    down[6], block = lax.optimization_barrier((tside_far, block))
    theirs, last = block_product(across, down, True)
    schur = (block + last) + swap(theirs, "k")
    return schur, side


def solution(mesh):
    torus = Mesh(mesh.devices.reshape(SIZES), AXES)
    placed = (P(ROW, None), P(), P(None, None, COL), P(None, COL), P(None, COL), P(ROW))


    return jax.shard_map(on_device, mesh=torus, in_specs=placed, out_specs=(P(ROW, COL), P(ROW)), check_vma=False)
```

```python
import math

import jax
import jax.numpy as jnp
from jax import lax
from jax.experimental import pallas as pl
from jax.experimental.pallas import tpu as pltpu
from jax.sharding import Mesh
from jax.sharding import PartitionSpec as P

AXES = ("z", "xl", "xh", "y", "k")
SIZES = (4, 2, 2, 4, 2)
ROW = ("z", "xl")
COL = ("xh", "y", "k")
F32 = jnp.float32
BF16 = jnp.bfloat16


norm_eps = 1e-06
diag_shift = 0.05

NB = 128
PG = 16


def halves(x):
    hi = x.astype(BF16)
    return hi, (x - hi.astype(F32)).astype(BF16)


def dot3(a, b, dims=((1,), (0,))):
    (ah, al), (bh, bl) = a, b
    d = lambda u, v: lax.dot_general(u, v, (dims, ((), ())), preferred_element_type=F32)
    return d(ah, bh) + (d(ah, bl) + d(al, bh))


def factor_block(x_ref, f_ref, gh_ref, gl_ref):
    row = lax.broadcasted_iota(jnp.int32, (PG, NB), 0)
    lane = lax.broadcasted_iota(jnp.int32, (NB, NB), 1)
    for g in range(NB // PG):
        lo = g * PG
        p0 = x_ref[lo : lo + PG, :NB]
        p1 = x_ref[lo : lo + PG, NB:]
        cols = [jnp.broadcast_to(p0[:, lo + j : lo + j + 1], (PG, NB)) for j in range(PG)]
        f1 = jnp.zeros_like(p1)
        for i in range(PG):
            up = lambda v: jnp.broadcast_to(v[i : i + 1, :], (PG, NB))
            piv = up(cols[i])
            inv = 1.0 / piv
            here = row == i
            a1 = up(p1)
            f1 = jnp.where(here, a1 * lax.rsqrt(piv), f1)
            a0 = up(p0) * inv
            a1 = a1 * inv
            ci = cols[i]
            for j in range(i + 1, PG):
                b = up(cols[j]) * inv
                cols[j] = jnp.where(here, b, cols[j] - ci * b)
            p0 = jnp.where(here, a0, p0 - ci * a0)
            p1 = jnp.where(here, a1, p1 - ci * a1)
        f_ref[lo : lo + PG, :] = f1
        if g + 1 < NB // PG:
            for half, v in ((slice(0, NB), p0), (slice(NB, 2 * NB), p1)):
                gh_ref[lo : lo + PG, half], gl_ref[lo : lo + PG, half] = halves(v)
            rest = slice(lo + PG, NB)
            n = NB - lo - PG
            inside = (lane[:n] >= lo) & (lane[:n] < lo + PG)
            left = halves(jnp.where(inside, x_ref[rest, :NB], 0.0))
            x_ref[rest, :] = x_ref[rest, :] - dot3(left, (gh_ref[...], gl_ref[...]))


def eliminate(t_ref, w_ref, first, x_ref, f_ref, gh_ref, gl_ref, yh_ref, yl_ref):
    n = t_ref.shape[1]
    gh_ref[...] = jnp.zeros_like(gh_ref)
    gl_ref[...] = jnp.zeros_like(gl_ref)
    eye = lax.broadcasted_iota(jnp.int32, (NB, NB), 0) == lax.broadcasted_iota(jnp.int32, (NB, NB), 1)
    ident = eye.astype(F32)
    wide = lax.broadcasted_iota(jnp.int32, (NB, n), 1)

    def step(b, carry):
        at = pl.multiple_of(first + b * NB, NB)
        mine = pl.ds(pl.multiple_of(b * NB, NB), NB)
        here = pl.ds(at, NB)
        x_ref[:, :NB] = t_ref[mine, here] + diag_shift * ident
        x_ref[:, NB:] = ident
        factor_block(x_ref, f_ref, gh_ref, gl_ref)
        linv = halves(f_ref[...])
        t_ref[mine, here] = ident
        y = dot3(linv, halves(t_ref[mine, :]))
        w_ref[mine, :] = jnp.where(wide < at + NB, y, 0.0)
        yh_ref[...], yl_ref[...] = halves(y)

        def below(r, c):
            rows = pl.ds(pl.multiple_of(r * NB, NB), NB)
            mult = dot3(halves(t_ref[rows, here]), linv, ((1,), (1,)))
            t_ref[rows, here] = jnp.zeros((NB, NB), F32)
            t_ref[rows, :] = t_ref[rows, :] - dot3(halves(mult), (yh_ref[...], yl_ref[...]))
            return c

        lax.fori_loop(b + 1, t_ref.shape[0] // NB, below, 0)
        return carry

    lax.fori_loop(0, w_ref.shape[0] // NB, step, 0)


def first_half(*refs):
    parts, (w_ref, out_ref, t_ref, *scratch, sems) = refs[:8], refs[8:]
    z, k = lax.axis_index("z"), lax.axis_index("k")
    copies = []
    for dk in range(2):
        for dz in range(4):
            i = dk * 4 + dz
            at = ((k + dk) % 2) * 512 + ((z + dz) % 4) * 128
            copies.append(pltpu.make_async_copy(parts[i], t_ref.at[pl.ds(pl.multiple_of(at, 128), 128)], sems.at[i]))
    for c in copies:
        c.start()
    for c in copies:
        c.wait()
    eliminate(t_ref, w_ref, 0, *scratch)
    out_ref[...] = t_ref[512:, :]


def later_part(first, a_ref, w_ref, *refs):
    done = w_ref.shape[0]
    (out_ref,), (t_ref, *scratch) = (refs[:1], refs[1:]) if first + done < 1024 else ((None,), refs)
    t_ref[...] = a_ref[...]
    eliminate(t_ref, w_ref, first, *scratch)
    if out_ref is not None:
        out_ref[...] = t_ref[done:, :]


FACTOR_SCRATCH = [
    pltpu.VMEM((NB, 2 * NB), F32),
    pltpu.VMEM((NB, NB), F32),
    pltpu.VMEM((NB, 2 * NB), BF16),
    pltpu.VMEM((NB, 2 * NB), BF16),
    pltpu.VMEM((NB, 1024), BF16),
    pltpu.VMEM((NB, 1024), BF16),
]
KERNEL_PARAMS = pltpu.CompilerParams(vmem_limit_bytes=40 * 1024 * 1024)


def factor_cost(flops):
    return pl.CostEstimate(flops=flops, transcendentals=0, bytes_accessed=8_000_000)


def lines(n):
    return jax.ShapeDtypeStruct((n, 1024), F32)


def start_inverse(parts):
    return pl.pallas_call(
        first_half,
        out_shape=(lines(512), lines(512)),
        in_specs=[pl.BlockSpec(memory_space=pl.ANY)] * 8,
        scratch_shapes=[pltpu.VMEM((1024, 1024), F32), *FACTOR_SCRATCH, pltpu.SemaphoreType.DMA((8,))],
        compiler_params=KERNEL_PARAMS,
        cost_estimate=factor_cost(15_000_000_000),
        name="inverse_first",
    )(*parts)


def go_on_inverse(rest, count):
    left = rest.shape[0]
    return pl.pallas_call(
        lambda *refs: later_part(1024 - left, *refs),
        out_shape=(lines(count), lines(left - count)) if left > count else (lines(count),),
        scratch_shapes=[pltpu.VMEM((left, 1024), F32), *FACTOR_SCRATCH],
        compiler_params=KERNEL_PARAMS,
        cost_estimate=factor_cost(5_000_000_000),
    )(rest)


def block_kernel(far, across, down, outs, a_ref, b_ref, sems):
    z, xl, xh, y, k = [lax.axis_index(a) for a in AXES]
    wanted = lambda d: ((d % 4 == (y + 2) % 4) | (d // 2 == (z + 2) % 4)) == far
    copies = []
    for i in range(8):
        step, flip = i % 4, i // 4
        if across[i] is not None:
            d = ((xh + flip) % 2) * 4 + (y + step) % 4
            copies.append((d, pltpu.make_async_copy(across[i], a_ref.at[d], sems.at[0, i])))
            d = ((z + step) % 4) * 2 + (xl + flip) % 2
            copies.append((d, pltpu.make_async_copy(down[i], b_ref.at[d], sems.at[1, i])))
    for d, c in copies:
        pl.when(wanted(d))(c.start)
    for out in outs:
        out[...] = jnp.zeros_like(out)
    for d, c in copies:
        pl.when(wanted(d))(c.wait)

    def one(d, carry):
        @pl.when(wanted(d))
        def _():
            for theirs, out in zip((1, 0), outs):
                b = b_ref[d, pl.ds(pl.multiple_of(((k + theirs) % 2) * 512, 512), 512), :]
                for r in range(0, 1024, 256):
                    out[r : r + 256, :] += outer(a_ref[d, r : r + 256, :], b)

        return carry

    lax.fori_loop(0, 8, one, 0)


BLOCK = jax.ShapeDtypeStruct((1024, 512), F32)


def block_product(across, down, far):
    ids = range(8) if far else [0, 1, 3, 4, 5, 7]
    n = len(ids)

    def body(*refs):
        a, b = [None] * 8, [None] * 8
        for at, i in enumerate(ids):
            a[i], b[i] = refs[at], refs[n + at]
        block_kernel(far, a, b, refs[2 * n : 2 * n + 2], *refs[2 * n + 2 :])

    return pl.pallas_call(
        body,
        out_shape=(BLOCK, BLOCK),
        in_specs=[pl.BlockSpec(memory_space=pl.ANY)] * (2 * n),
        scratch_shapes=[
            pltpu.VMEM((8, 1024, 512), BF16),
            pltpu.VMEM((8, 1024, 512), BF16),
            pltpu.SemaphoreType.DMA((2, 8)),
        ],
        compiler_params=KERNEL_PARAMS,
        cost_estimate=pl.CostEstimate(flops=4_300_000_000, transcendentals=0, bytes_accessed=14_000_000),
        name="block_far" if far else "block_near",
    )(*[across[i] for i in ids], *[down[i] for i in ids])


def swap(x, axis):
    return lax.ppermute(x, axis, [(0, 1), (1, 0)])


def shift(x, axis, by):
    n = lax.axis_size(axis)
    return lax.ppermute(x, axis, [(i, (i + by) % n) for i in range(n)])


def send(x, axis, src, dst):
    return lax.ppermute(x, axis, [(src, dst)])


def after(x, *others):
    return lax.optimization_barrier((x, *others))[0]


def gather2(x, axis):
    other = swap(x, axis)
    first = lax.axis_index(axis) == 0
    return jnp.stack([jnp.where(first, x, other), jnp.where(first, other, x)])


def ring4(x, axis):
    return [x, shift(x, axis, -1), shift(x, axis, 2), shift(x, axis, 1)]


def in_order(parts, axis):
    size = parts[0].shape[0]
    out = jnp.zeros((4 * size,) + parts[0].shape[1:], parts[0].dtype)
    for step, part in enumerate(parts):
        at = (lax.axis_index(axis) + step) % 4
        out = lax.dynamic_update_slice_in_dim(out, part, at * size, 0)
    return out


def scatter2(x, axis):
    me = lax.axis_index(axis)
    other = swap(lax.dynamic_index_in_dim(x, 1 - me, 0, False), axis)
    return lax.dynamic_index_in_dim(x, me, 0, False) + other


def scatter4(x, axis):
    me = lax.axis_index(axis)
    pick = lambda ahead: lax.dynamic_index_in_dim(x, (me + ahead) % 4, 0, False)
    return (pick(0) + shift(pick(2), axis, 2)) + (shift(pick(1), axis, 1) + shift(pick(3), axis, -1))


def first_of_pair(x):
    return jnp.where(lax.axis_index("xl") == 0, x, send(x, "xl", 0, 1))


def first_of_ring(x):
    return lax.select_n(lax.axis_index("z"), x, send(x, "z", 0, 1), send(x, "z", 0, 2), send(x, "z", 0, 3))


def transpose_chips(x):
    pairs = []
    for d in range(math.prod(SIZES)):
        k, c, r = d % 2, (d // 2) % 8, d // 16
        pairs.append((d, (c * 8 + r) * 2 + k))
    return lax.ppermute(x, AXES, pairs)


def sum_rows(x):
    x = x + swap(x, "xl")
    x = x + lax.ppermute(x, "z", [(i, i ^ 1) for i in range(4)])
    return x + lax.ppermute(x, "z", [(i, i ^ 2) for i in range(4)])


def embed(occupations, table):
    onehot = jnp.concatenate([(occupations == v).astype(F32) for v in range(3)], axis=1)
    embedded = jnp.dot(onehot, table, precision=lax.Precision.HIGH, preferred_element_type=F32)
    return embedded * lax.rsqrt(jnp.mean(embedded * embedded, axis=-1, keepdims=True) + norm_eps)


def log_derivatives(embedded, weights, biases, heads):
    blocks = []
    for p in range(2):
        hidden = jnp.dot(embedded, weights[p], precision=lax.Precision.HIGH, preferred_element_type=F32)
        blocks.append(heads[p] * jax.nn.sigmoid(hidden + biases[p]))
    return jnp.concatenate(blocks, axis=1)


def outer(a, b):
    return lax.dot_general(a, b, (((1,), (1,)), ((), ())), preferred_element_type=F32)


def outer3(a, b):
    return lax.dot_general(
        a, b, (((1,), (1,)), ((), ())), precision=lax.Precision.HIGH, preferred_element_type=F32
    )


def on_device(occupations, table, weights, biases, heads, energies):
    rows = occupations.shape[0]
    total = rows * 8
    cols = total // 16
    z, xl, xh, y, core = [lax.axis_index(a) for a in AXES]
    row, chip_col = z * 2 + xl, xh * 4 + y
    par = weights.shape[0] * weights.shape[2]

    side_parts, remains = [], energies.reshape(-1, occupations.shape[1])
    for _ in range(3):
        rounded = lax.reduce_precision(remains, 8, 7)
        side_parts.append(rounded.astype(BF16))
        remains = remains - rounded
    pair_occ = first_of_pair(jnp.concatenate([occupations.astype(BF16), *side_parts]))
    embedded = embed(occupations, table)
    first_occ = after(first_of_ring(pair_occ), embedded)
    first_side = jnp.sum(first_occ[rows:].astype(F32).reshape(3, rows), axis=0, keepdims=True)
    first_occ = first_occ[:rows]
    derivs = log_derivatives(embedded, weights, biases, heads)
    sums = jnp.sum(derivs, axis=0, keepdims=True)
    first_embedded = embed(after(first_occ, sums), table)
    first_derivs = log_derivatives(first_embedded, weights, biases, heads)
    mean = sum_rows(sums) / total
    center = lambda d: ((d - mean) * (1.0 / math.sqrt(total))).astype(BF16)
    own, first = center(derivs), center(first_derivs)

    eye = lambda r, c, r0, c0: jnp.where(
        (lax.broadcasted_iota(jnp.int32, (r, c), 0) + r0) == (lax.broadcasted_iota(jnp.int32, (r, c), 1) + c0),
        diag_shift,
        0.0,
    ).astype(F32)

    pick = first.reshape(2, 4, 4, 2, 16, par)
    pick = lax.dynamic_index_in_dim(lax.dynamic_index_in_dim(pick, z, 1, False), xl, 2, False)
    slab = outer(pick.reshape(128, par), first).reshape(2, 4, 2, 8, rows)
    slab = scatter2(slab, "k")
    panel = outer(after(own, slab), first).reshape(2, 4, 2, rows // 16, rows)
    slab = scatter4(slab, "y")
    panel = scatter2(panel, "k")
    slab = scatter2(slab, "xh")
    slab = gather2(gather2(slab, "xh"), "xl")
    slab = in_order(ring4(slab.reshape(32, rows), "y"), "y")
    parts = ring4(slab, "z")
    parts = parts + [swap(p, "k") for p in parts]
    own_y = after(own, slab)
    turned = transpose_chips(own_y)
    beside = swap(own_y, "xh")
    panel = scatter4(after(panel, slab), "y")
    own_next, own_prev = shift(own_y, "y", -1), shift(own_y, "y", 1)

    low, rest = start_inverse(parts)
    mid, rest = go_on_inverse(rest, 256)
    panel, turned, beside, own_prev, rest = lax.optimization_barrier((panel, turned, beside, own_prev, rest))
    panel = scatter2(panel, "xh")
    turned_next, turned_prev = shift(turned, "z", -1), shift(turned, "z", 1)
    turned_side = swap(turned, "xl")
    side_next, side_prev = shift(beside, "y", -1), shift(beside, "y", 1)
    own_far = shift(own_prev, "y", 1)

    (high,) = go_on_inverse(rest, 256)
    panel, high = lax.optimization_barrier((panel, high))
    mine = gather2(panel, "xh").reshape(rows // 8, rows)
    other = transpose_chips(panel)
    mine = ring4(mine, "y")
    turned_side = after(turned_side, high)
    tside_next, tside_prev = (shift(turned_side, "z", -1), shift(turned_side, "z", 1))
    other = gather2(other, "xl").reshape(rows // 8, rows)
    other = ring4(other, "z")
    turned_far = shift(after(turned_prev, high), "z", 1)
    side_far = shift(after(side_next, high), "y", -1)
    tside_far = shift(tside_next, "z", -1)

    across = [own, own_next, own_far, own_prev, beside, side_next, side_far, side_prev]
    down = [turned, turned_next, turned_far, turned_prev, turned_side, tside_next, tside_far, tside_prev]
    theirs, block = block_product(across, down, False)
    block = block + swap(theirs, "k")

    mine = gather2(in_order(mine, "y"), "k").reshape(rows, rows)
    other = in_order(other, "z").reshape(2, 4, rows // 16, rows).transpose(1, 0, 2, 3).reshape(cols, rows)
    mine = mine + eye(rows, rows, row * rows, 0)
    other = other + eye(cols, rows, chip_col * rows + core * cols, 0)
    inverse = [low[:, :512], mid[:, :768], high]
    left = jnp.concatenate([outer3(mine[:, : w.shape[1]], w) for w in inverse], 1)
    right = jnp.concatenate([outer3(other[:, : w.shape[1]], w) for w in inverse], 1)
    exact = lambda a, b: lax.dot_general(
        a, b, (((1,), (1,)), ((), ())), precision=lax.Precision.HIGHEST, preferred_element_type=F32
    )
    solved = jnp.concatenate([exact(first_side[:, : w.shape[1]], w) for w in inverse], 1)
    side = energies - jnp.sum(left * solved, axis=1)
    side = jnp.where(row == 0, solved[0], side)
    block = (block + eye(rows, cols, row * rows, chip_col * rows + core * cols)) - outer3(left, right)

    down[6], block = lax.optimization_barrier((tside_far, block))
    theirs, last = block_product(across, down, True)
    schur = (block + last) + swap(theirs, "k")
    return schur, side


def solution(mesh):
    torus = Mesh(mesh.devices.reshape(SIZES), AXES)
    placed = (P(ROW, None), P(), P(None, None, COL), P(None, COL), P(None, COL), P(ROW))


    return jax.shard_map(on_device, mesh=torus, in_specs=placed, out_specs=(P(ROW, COL), P(ROW)), check_vma=False)
```

```python
import math

import jax
import jax.numpy as jnp
from jax import lax
from jax.experimental import pallas as pl
from jax.experimental.pallas import tpu as pltpu
from jax.sharding import Mesh
from jax.sharding import PartitionSpec as P

AXES = ("z", "xl", "xh", "y", "k")
SIZES = (4, 2, 2, 4, 2)
ROW = ("z", "xl")
COL = ("xh", "y", "k")
F32 = jnp.float32
BF16 = jnp.bfloat16


norm_eps = 1e-06
diag_shift = 0.05

NB = 128
PG = 16


def halves(x):
    hi = x.astype(BF16)
    return hi, (x - hi.astype(F32)).astype(BF16)


def dot3(a, b, dims=((1,), (0,))):
    (ah, al), (bh, bl) = a, b
    d = lambda u, v: lax.dot_general(u, v, (dims, ((), ())), preferred_element_type=F32)
    return d(ah, bh) + (d(ah, bl) + d(al, bh))


def factor_block(x_ref, f_ref, gh_ref, gl_ref):
    row = lax.broadcasted_iota(jnp.int32, (PG, NB), 0)
    lane = lax.broadcasted_iota(jnp.int32, (NB, NB), 1)
    for g in range(NB // PG):
        lo = g * PG
        p0 = x_ref[lo : lo + PG, :NB]
        p1 = x_ref[lo : lo + PG, NB:]
        cols = [jnp.broadcast_to(p0[:, lo + j : lo + j + 1], (PG, NB)) for j in range(PG)]
        f1 = jnp.zeros_like(p1)
        for i in range(PG):
            up = lambda v: jnp.broadcast_to(v[i : i + 1, :], (PG, NB))
            piv = up(cols[i])
            inv = 1.0 / piv
            here = row == i
            a1 = up(p1)
            f1 = jnp.where(here, a1 * lax.rsqrt(piv), f1)
            a0 = up(p0) * inv
            a1 = a1 * inv
            ci = cols[i]
            for j in range(i + 1, PG):
                b = up(cols[j]) * inv
                cols[j] = jnp.where(here, b, cols[j] - ci * b)
            p0 = jnp.where(here, a0, p0 - ci * a0)
            p1 = jnp.where(here, a1, p1 - ci * a1)
        f_ref[lo : lo + PG, :] = f1
        if g + 1 < NB // PG:
            for half, v in ((slice(0, NB), p0), (slice(NB, 2 * NB), p1)):
                gh_ref[lo : lo + PG, half], gl_ref[lo : lo + PG, half] = halves(v)
            rest = slice(lo + PG, NB)
            n = NB - lo - PG
            inside = (lane[:n] >= lo) & (lane[:n] < lo + PG)
            left = halves(jnp.where(inside, x_ref[rest, :NB], 0.0))
            x_ref[rest, :] = x_ref[rest, :] - dot3(left, (gh_ref[...], gl_ref[...]))


def eliminate(t_ref, w_ref, first, x_ref, f_ref, gh_ref, gl_ref, yh_ref, yl_ref):
    n = t_ref.shape[1]
    gh_ref[...] = jnp.zeros_like(gh_ref)
    gl_ref[...] = jnp.zeros_like(gl_ref)
    eye = lax.broadcasted_iota(jnp.int32, (NB, NB), 0) == lax.broadcasted_iota(jnp.int32, (NB, NB), 1)
    ident = eye.astype(F32)
    wide = lax.broadcasted_iota(jnp.int32, (NB, n), 1)

    def step(b, carry):
        at = pl.multiple_of(first + b * NB, NB)
        mine = pl.ds(pl.multiple_of(b * NB, NB), NB)
        here = pl.ds(at, NB)
        x_ref[:, :NB] = t_ref[mine, here] + diag_shift * ident
        x_ref[:, NB:] = ident
        factor_block(x_ref, f_ref, gh_ref, gl_ref)
        linv = halves(f_ref[...])
        t_ref[mine, here] = ident
        y = dot3(linv, halves(t_ref[mine, :]))
        w_ref[mine, :] = jnp.where(wide < at + NB, y, 0.0)
        yh_ref[...], yl_ref[...] = halves(y)

        def below(r, c):
            rows = pl.ds(pl.multiple_of(r * NB, NB), NB)
            mult = dot3(halves(t_ref[rows, here]), linv, ((1,), (1,)))
            t_ref[rows, here] = jnp.zeros((NB, NB), F32)
            t_ref[rows, :] = t_ref[rows, :] - dot3(halves(mult), (yh_ref[...], yl_ref[...]))
            return c

        lax.fori_loop(b + 1, t_ref.shape[0] // NB, below, 0)
        return carry

    lax.fori_loop(0, w_ref.shape[0] // NB, step, 0)


def first_half(*refs):
    parts, (w_ref, out_ref, t_ref, *scratch, sems) = refs[:8], refs[8:]
    z, k = lax.axis_index("z"), lax.axis_index("k")
    copies = []
    for dk in range(2):
        for dz in range(4):
            i = dk * 4 + dz
            at = ((k + dk) % 2) * 512 + ((z + dz) % 4) * 128
            copies.append(pltpu.make_async_copy(parts[i], t_ref.at[pl.ds(pl.multiple_of(at, 128), 128)], sems.at[i]))
    for c in copies:
        c.start()
    for c in copies:
        c.wait()
    eliminate(t_ref, w_ref, 0, *scratch)
    out_ref[...] = t_ref[512:, :]


def later_part(first, a_ref, w_ref, *refs):
    done = w_ref.shape[0]
    (out_ref,), (t_ref, *scratch) = (refs[:1], refs[1:]) if first + done < 1024 else ((None,), refs)
    t_ref[...] = a_ref[...]
    eliminate(t_ref, w_ref, first, *scratch)
    if out_ref is not None:
        out_ref[...] = t_ref[done:, :]


FACTOR_SCRATCH = [
    pltpu.VMEM((NB, 2 * NB), F32),
    pltpu.VMEM((NB, NB), F32),
    pltpu.VMEM((NB, 2 * NB), BF16),
    pltpu.VMEM((NB, 2 * NB), BF16),
    pltpu.VMEM((NB, 1024), BF16),
    pltpu.VMEM((NB, 1024), BF16),
]
KERNEL_PARAMS = pltpu.CompilerParams(vmem_limit_bytes=40 * 1024 * 1024)


def factor_cost(flops):
    return pl.CostEstimate(flops=flops, transcendentals=0, bytes_accessed=8_000_000)


def lines(n):
    return jax.ShapeDtypeStruct((n, 1024), F32)


def start_inverse(parts):
    return pl.pallas_call(
        first_half,
        out_shape=(lines(512), lines(512)),
        in_specs=[pl.BlockSpec(memory_space=pl.ANY)] * 8,
        scratch_shapes=[pltpu.VMEM((1024, 1024), F32), *FACTOR_SCRATCH, pltpu.SemaphoreType.DMA((8,))],
        compiler_params=KERNEL_PARAMS,
        cost_estimate=factor_cost(15_000_000_000),
        name="inverse_first",
    )(*parts)


def go_on_inverse(rest, count):
    left = rest.shape[0]
    return pl.pallas_call(
        lambda *refs: later_part(1024 - left, *refs),
        out_shape=(lines(count), lines(left - count)) if left > count else (lines(count),),
        scratch_shapes=[pltpu.VMEM((left, 1024), F32), *FACTOR_SCRATCH],
        compiler_params=KERNEL_PARAMS,
        cost_estimate=factor_cost(5_000_000_000),
    )(rest)


def block_kernel(far, across, down, outs, a_ref, b_ref, sems):
    z, xl, xh, y, k = [lax.axis_index(a) for a in AXES]
    wanted = lambda d: ((d % 4 == (y + 2) % 4) | (d // 2 == (z + 2) % 4)) == far
    copies = []
    for i in range(8):
        step, flip = i % 4, i // 4
        if across[i] is not None:
            d = ((xh + flip) % 2) * 4 + (y + step) % 4
            copies.append((d, pltpu.make_async_copy(across[i], a_ref.at[d], sems.at[0, i])))
            d = ((z + step) % 4) * 2 + (xl + flip) % 2
            copies.append((d, pltpu.make_async_copy(down[i], b_ref.at[d], sems.at[1, i])))
    for d, c in copies:
        pl.when(wanted(d))(c.start)
    for out in outs:
        out[...] = jnp.zeros_like(out)
    for d, c in copies:
        pl.when(wanted(d))(c.wait)

    def one(d, carry):
        @pl.when(wanted(d))
        def _():
            for theirs, out in zip((1, 0), outs):
                b = b_ref[d, pl.ds(pl.multiple_of(((k + theirs) % 2) * 512, 512), 512), :]
                for r in range(0, 1024, 256):
                    out[r : r + 256, :] += outer(a_ref[d, r : r + 256, :], b)

        return carry

    lax.fori_loop(0, 8, one, 0)


BLOCK = jax.ShapeDtypeStruct((1024, 512), F32)


def block_product(across, down, far):
    ids = range(8) if far else [0, 1, 3, 4, 5, 7]
    n = len(ids)

    def body(*refs):
        a, b = [None] * 8, [None] * 8
        for at, i in enumerate(ids):
            a[i], b[i] = refs[at], refs[n + at]
        block_kernel(far, a, b, refs[2 * n : 2 * n + 2], *refs[2 * n + 2 :])

    return pl.pallas_call(
        body,
        out_shape=(BLOCK, BLOCK),
        in_specs=[pl.BlockSpec(memory_space=pl.ANY)] * (2 * n),
        scratch_shapes=[
            pltpu.VMEM((8, 1024, 512), BF16),
            pltpu.VMEM((8, 1024, 512), BF16),
            pltpu.SemaphoreType.DMA((2, 8)),
        ],
        compiler_params=KERNEL_PARAMS,
        cost_estimate=pl.CostEstimate(flops=4_300_000_000, transcendentals=0, bytes_accessed=14_000_000),
        name="block_far" if far else "block_near",
    )(*[across[i] for i in ids], *[down[i] for i in ids])


def swap(x, axis):
    return lax.ppermute(x, axis, [(0, 1), (1, 0)])


def shift(x, axis, by):
    n = lax.axis_size(axis)
    return lax.ppermute(x, axis, [(i, (i + by) % n) for i in range(n)])


def send(x, axis, src, dst):
    return lax.ppermute(x, axis, [(src, dst)])


def after(x, *others):
    return lax.optimization_barrier((x, *others))[0]


def gather2(x, axis):
    other = swap(x, axis)
    first = lax.axis_index(axis) == 0
    return jnp.stack([jnp.where(first, x, other), jnp.where(first, other, x)])


def ring4(x, axis):
    return [x, shift(x, axis, -1), shift(x, axis, 2), shift(x, axis, 1)]


def in_order(parts, axis):
    size = parts[0].shape[0]
    out = jnp.zeros((4 * size,) + parts[0].shape[1:], parts[0].dtype)
    for step, part in enumerate(parts):
        at = (lax.axis_index(axis) + step) % 4
        out = lax.dynamic_update_slice_in_dim(out, part, at * size, 0)
    return out


def scatter2(x, axis):
    me = lax.axis_index(axis)
    other = swap(lax.dynamic_index_in_dim(x, 1 - me, 0, False), axis)
    return lax.dynamic_index_in_dim(x, me, 0, False) + other


def scatter4(x, axis):
    me = lax.axis_index(axis)
    pick = lambda ahead: lax.dynamic_index_in_dim(x, (me + ahead) % 4, 0, False)
    return (pick(0) + shift(pick(2), axis, 2)) + (shift(pick(1), axis, 1) + shift(pick(3), axis, -1))


def first_of_pair(x):
    return jnp.where(lax.axis_index("xl") == 0, x, send(x, "xl", 0, 1))


def first_of_ring(x):
    return lax.select_n(lax.axis_index("z"), x, send(x, "z", 0, 1), send(x, "z", 0, 2), send(x, "z", 0, 3))


def transpose_chips(x):
    pairs = []
    for d in range(math.prod(SIZES)):
        k, c, r = d % 2, (d // 2) % 8, d // 16
        pairs.append((d, (c * 8 + r) * 2 + k))
    return lax.ppermute(x, AXES, pairs)


def sum_rows(x):
    x = x + swap(x, "xl")
    x = x + lax.ppermute(x, "z", [(i, i ^ 1) for i in range(4)])
    return x + lax.ppermute(x, "z", [(i, i ^ 2) for i in range(4)])


def embed(occupations, table):
    onehot = jnp.concatenate([(occupations == v).astype(F32) for v in range(3)], axis=1)
    embedded = jnp.dot(onehot, table, precision=lax.Precision.HIGH, preferred_element_type=F32)
    return embedded * lax.rsqrt(jnp.mean(embedded * embedded, axis=-1, keepdims=True) + norm_eps)


def log_derivatives(embedded, weights, biases, heads):
    blocks = []
    for p in range(2):
        hidden = jnp.dot(embedded, weights[p], precision=lax.Precision.HIGH, preferred_element_type=F32)
        blocks.append(heads[p] * jax.nn.sigmoid(hidden + biases[p]))
    return jnp.concatenate(blocks, axis=1)


def outer(a, b):
    return lax.dot_general(a, b, (((1,), (1,)), ((), ())), preferred_element_type=F32)


def outer3(a, b):
    return lax.dot_general(
        a, b, (((1,), (1,)), ((), ())), precision=lax.Precision.HIGH, preferred_element_type=F32
    )


def on_device(occupations, table, weights, biases, heads, energies):
    rows = occupations.shape[0]
    total = rows * 8
    cols = total // 16
    z, xl, xh, y, core = [lax.axis_index(a) for a in AXES]
    row, chip_col = z * 2 + xl, xh * 4 + y
    par = weights.shape[0] * weights.shape[2]

    side_parts, remains = [], energies.reshape(-1, occupations.shape[1])
    for _ in range(3):
        rounded = lax.reduce_precision(remains, 8, 7)
        side_parts.append(rounded.astype(BF16))
        remains = remains - rounded
    pair_occ = first_of_pair(jnp.concatenate([occupations.astype(BF16), *side_parts]))
    embedded = embed(occupations, table)
    first_occ = after(first_of_ring(pair_occ), embedded)
    first_side = jnp.sum(first_occ[rows:].astype(F32).reshape(3, rows), axis=0, keepdims=True)
    first_occ = first_occ[:rows]
    derivs = log_derivatives(embedded, weights, biases, heads)
    sums = jnp.sum(derivs, axis=0, keepdims=True)
    first_embedded = embed(after(first_occ, sums), table)
    first_derivs = log_derivatives(first_embedded, weights, biases, heads)
    mean = sum_rows(sums) / total
    center = lambda d: ((d - mean) * (1.0 / math.sqrt(total))).astype(BF16)
    own, first = center(derivs), center(first_derivs)

    eye = lambda r, c, r0, c0: jnp.where(
        (lax.broadcasted_iota(jnp.int32, (r, c), 0) + r0) == (lax.broadcasted_iota(jnp.int32, (r, c), 1) + c0),
        diag_shift,
        0.0,
    ).astype(F32)

    pick = first.reshape(2, 4, 4, 2, 16, par)
    pick = lax.dynamic_index_in_dim(lax.dynamic_index_in_dim(pick, z, 1, False), xl, 2, False)
    slab = outer(pick.reshape(128, par), first).reshape(2, 4, 2, 8, rows)
    own_x = after(own, slab)
    turned = transpose_chips(own_x)
    slab = scatter2(slab, "k")
    panel = outer(own_x, first).reshape(2, 4, 2, rows // 16, rows)
    panel = scatter2(panel, "k")
    slab = scatter4(slab, "y")
    turned_next, turned_prev = shift(turned, "z", -1), shift(turned, "z", 1)
    slab = scatter2(slab, "xh")
    slab = gather2(gather2(slab, "xh"), "xl")
    beside = swap(after(own, slab), "xh")
    turned_side = swap(after(turned, slab), "xl")
    slab = in_order(ring4(slab.reshape(32, rows), "y"), "y")
    panel = scatter4(after(panel, slab), "y")
    own_y = after(own, slab)
    own_next, own_prev = shift(own_y, "y", -1), shift(own_y, "y", 1)
    parts = ring4(slab, "z")
    parts = parts + [swap(p, "k") for p in parts]
    turned_side, beside, *parts = lax.optimization_barrier((turned_side, beside, *parts))
    side_next, side_prev = shift(beside, "y", -1), shift(beside, "y", 1)
    tside_next, tside_prev = (shift(turned_side, "z", -1), shift(turned_side, "z", 1))
    panel = scatter2(after(panel, *parts), "xh")

    low, rest = start_inverse(parts)
    panel, side_next, tside_next, own_prev, turned_prev, rest = lax.optimization_barrier(
        (panel, side_next, tside_next, own_prev, turned_prev, rest)
    )
    mine = gather2(panel, "xh").reshape(rows // 8, rows)
    panel_turned = transpose_chips(panel)
    own_far = shift(own_prev, "y", 1)
    turned_far = shift(turned_prev, "z", 1)
    side_far = shift(side_next, "y", -1)
    tside_far = shift(tside_next, "z", -1)

    mid, rest = go_on_inverse(rest, 256)
    panel_turned, mine, rest = lax.optimization_barrier((panel_turned, mine, rest))
    mine = ring4(mine, "y")
    other = gather2(panel_turned, "xl").reshape(rows // 8, rows)

    (high,) = go_on_inverse(rest, 256)
    other, high = lax.optimization_barrier((other, high))
    other = ring4(other, "z")

    across = [own, own_next, own_far, own_prev, beside, side_next, side_far, side_prev]
    down = [turned, turned_next, turned_far, turned_prev, turned_side, tside_next, tside_far, tside_prev]
    theirs, block = block_product(across, down, False)
    block = block + swap(theirs, "k")

    mine = gather2(in_order(mine, "y"), "k").reshape(rows, rows)
    other = in_order(other, "z").reshape(2, 4, rows // 16, rows).transpose(1, 0, 2, 3).reshape(cols, rows)
    mine = mine + eye(rows, rows, row * rows, 0)
    other = other + eye(cols, rows, chip_col * rows + core * cols, 0)
    inverse = [low[:, :512], mid[:, :768], high]
    left = jnp.concatenate([outer3(mine[:, : w.shape[1]], w) for w in inverse], 1)
    right = jnp.concatenate([outer3(other[:, : w.shape[1]], w) for w in inverse], 1)
    exact = lambda a, b: lax.dot_general(
        a, b, (((1,), (1,)), ((), ())), precision=lax.Precision.HIGHEST, preferred_element_type=F32
    )
    solved = jnp.concatenate([exact(first_side[:, : w.shape[1]], w) for w in inverse], 1)
    side = energies - jnp.sum(left * solved, axis=1)
    side = jnp.where(row == 0, solved[0], side)
    block = (block + eye(rows, cols, row * rows, chip_col * rows + core * cols)) - outer3(left, right)

    down[6], block = lax.optimization_barrier((tside_far, block))
    theirs, last = block_product(across, down, True)
    schur = (block + last) + swap(theirs, "k")
    return schur, side


def solution(mesh):
    torus = Mesh(mesh.devices.reshape(SIZES), AXES)
    placed = (P(ROW, None), P(), P(None, None, COL), P(None, COL), P(None, COL), P(ROW))


    return jax.shard_map(on_device, mesh=torus, in_specs=placed, out_specs=(P(ROW, COL), P(ROW)), check_vma=False)
```

```python
import math

import jax
import jax.numpy as jnp
from jax import lax
from jax.experimental import pallas as pl
from jax.experimental.pallas import tpu as pltpu
from jax.sharding import Mesh
from jax.sharding import PartitionSpec as P

AXES = ("z", "xl", "xh", "y", "k")
SIZES = (4, 2, 2, 4, 2)
ROW = ("z", "xl")
COL = ("xh", "y", "k")
F32 = jnp.float32
BF16 = jnp.bfloat16


norm_eps = 1e-06
diag_shift = 0.05

NB = 128
PG = 16


def halves(x):
    hi = x.astype(BF16)
    return hi, (x - hi.astype(F32)).astype(BF16)


def dot3(a, b, dims=((1,), (0,))):
    (ah, al), (bh, bl) = a, b
    d = lambda u, v: lax.dot_general(u, v, (dims, ((), ())), preferred_element_type=F32)
    return d(ah, bh) + (d(ah, bl) + d(al, bh))


def factor_block(x_ref, f_ref, gh_ref, gl_ref):
    row = lax.broadcasted_iota(jnp.int32, (PG, NB), 0)
    lane = lax.broadcasted_iota(jnp.int32, (NB, NB), 1)
    for g in range(NB // PG):
        lo = g * PG
        p0 = x_ref[lo : lo + PG, :NB]
        p1 = x_ref[lo : lo + PG, NB:]
        cols = [jnp.broadcast_to(p0[:, lo + j : lo + j + 1], (PG, NB)) for j in range(PG)]
        f1 = jnp.zeros_like(p1)
        for i in range(PG):
            up = lambda v: jnp.broadcast_to(v[i : i + 1, :], (PG, NB))
            piv = up(cols[i])
            inv = 1.0 / piv
            here = row == i
            a1 = up(p1)
            f1 = jnp.where(here, a1 * lax.rsqrt(piv), f1)
            a0 = up(p0) * inv
            a1 = a1 * inv
            ci = cols[i]
            for j in range(i + 1, PG):
                b = up(cols[j]) * inv
                cols[j] = jnp.where(here, b, cols[j] - ci * b)
            p0 = jnp.where(here, a0, p0 - ci * a0)
            p1 = jnp.where(here, a1, p1 - ci * a1)
        f_ref[lo : lo + PG, :] = f1
        if g + 1 < NB // PG:
            for half, v in ((slice(0, NB), p0), (slice(NB, 2 * NB), p1)):
                gh_ref[lo : lo + PG, half], gl_ref[lo : lo + PG, half] = halves(v)
            rest = slice(lo + PG, NB)
            n = NB - lo - PG
            inside = (lane[:n] >= lo) & (lane[:n] < lo + PG)
            left = halves(jnp.where(inside, x_ref[rest, :NB], 0.0))
            x_ref[rest, :] = x_ref[rest, :] - dot3(left, (gh_ref[...], gl_ref[...]))


def eliminate(t_ref, w_ref, first, x_ref, f_ref, gh_ref, gl_ref, yh_ref, yl_ref):
    n = t_ref.shape[1]
    gh_ref[...] = jnp.zeros_like(gh_ref)
    gl_ref[...] = jnp.zeros_like(gl_ref)
    eye = lax.broadcasted_iota(jnp.int32, (NB, NB), 0) == lax.broadcasted_iota(jnp.int32, (NB, NB), 1)
    ident = eye.astype(F32)
    wide = lax.broadcasted_iota(jnp.int32, (NB, n), 1)

    def step(b, carry):
        at = pl.multiple_of(first + b * NB, NB)
        mine = pl.ds(pl.multiple_of(b * NB, NB), NB)
        here = pl.ds(at, NB)
        x_ref[:, :NB] = t_ref[mine, here] + diag_shift * ident
        x_ref[:, NB:] = ident
        factor_block(x_ref, f_ref, gh_ref, gl_ref)
        linv = halves(f_ref[...])
        t_ref[mine, here] = ident
        y = dot3(linv, halves(t_ref[mine, :]))
        w_ref[mine, :] = jnp.where(wide < at + NB, y, 0.0)
        yh_ref[...], yl_ref[...] = halves(y)

        def below(r, c):
            rows = pl.ds(pl.multiple_of(r * NB, NB), NB)
            mult = dot3(halves(t_ref[rows, here]), linv, ((1,), (1,)))
            t_ref[rows, here] = jnp.zeros((NB, NB), F32)
            t_ref[rows, :] = t_ref[rows, :] - dot3(halves(mult), (yh_ref[...], yl_ref[...]))
            return c

        lax.fori_loop(b + 1, t_ref.shape[0] // NB, below, 0)
        return carry

    lax.fori_loop(0, w_ref.shape[0] // NB, step, 0)


def first_half(*refs):
    parts, (w_ref, out_ref, t_ref, *scratch, sems) = refs[:8], refs[8:]
    z, k = lax.axis_index("z"), lax.axis_index("k")
    copies = []
    for dk in range(2):
        for dz in range(4):
            i = dk * 4 + dz
            at = ((k + dk) % 2) * 512 + ((z + dz) % 4) * 128
            copies.append(pltpu.make_async_copy(parts[i], t_ref.at[pl.ds(pl.multiple_of(at, 128), 128)], sems.at[i]))
    for c in copies:
        c.start()
    for c in copies:
        c.wait()
    eliminate(t_ref, w_ref, 0, *scratch)
    out_ref[...] = t_ref[512:, :]


def later_part(first, a_ref, w_ref, *refs):
    done = w_ref.shape[0]
    (out_ref,), (t_ref, *scratch) = (refs[:1], refs[1:]) if first + done < 1024 else ((None,), refs)
    t_ref[...] = a_ref[...]
    eliminate(t_ref, w_ref, first, *scratch)
    if out_ref is not None:
        out_ref[...] = t_ref[done:, :]


FACTOR_SCRATCH = [
    pltpu.VMEM((NB, 2 * NB), F32),
    pltpu.VMEM((NB, NB), F32),
    pltpu.VMEM((NB, 2 * NB), BF16),
    pltpu.VMEM((NB, 2 * NB), BF16),
    pltpu.VMEM((NB, 1024), BF16),
    pltpu.VMEM((NB, 1024), BF16),
]
KERNEL_PARAMS = pltpu.CompilerParams(vmem_limit_bytes=40 * 1024 * 1024)


def factor_cost(flops):
    return pl.CostEstimate(flops=flops, transcendentals=0, bytes_accessed=8_000_000)


def lines(n):
    return jax.ShapeDtypeStruct((n, 1024), F32)


def start_inverse(parts):
    return pl.pallas_call(
        first_half,
        out_shape=(lines(512), lines(512)),
        in_specs=[pl.BlockSpec(memory_space=pl.ANY)] * 8,
        scratch_shapes=[pltpu.VMEM((1024, 1024), F32), *FACTOR_SCRATCH, pltpu.SemaphoreType.DMA((8,))],
        compiler_params=KERNEL_PARAMS,
        cost_estimate=factor_cost(15_000_000_000),
        name="inverse_first",
    )(*parts)


def go_on_inverse(rest, count):
    left = rest.shape[0]
    return pl.pallas_call(
        lambda *refs: later_part(1024 - left, *refs),
        out_shape=(lines(count), lines(left - count)) if left > count else (lines(count),),
        scratch_shapes=[pltpu.VMEM((left, 1024), F32), *FACTOR_SCRATCH],
        compiler_params=KERNEL_PARAMS,
        cost_estimate=factor_cost(5_000_000_000),
    )(rest)


def block_kernel(far, across, down, outs, a_ref, b_ref, sems):
    z, xl, xh, y, k = [lax.axis_index(a) for a in AXES]
    wanted = lambda d: ((d % 4 == (y + 2) % 4) | (d // 2 == (z + 2) % 4)) == far
    copies = []
    for i in range(8):
        step, flip = i % 4, i // 4
        if across[i] is not None:
            d = ((xh + flip) % 2) * 4 + (y + step) % 4
            copies.append((d, pltpu.make_async_copy(across[i], a_ref.at[d], sems.at[0, i])))
            d = ((z + step) % 4) * 2 + (xl + flip) % 2
            copies.append((d, pltpu.make_async_copy(down[i], b_ref.at[d], sems.at[1, i])))
    for d, c in copies:
        pl.when(wanted(d))(c.start)
    for out in outs:
        out[...] = jnp.zeros_like(out)
    for d, c in copies:
        pl.when(wanted(d))(c.wait)

    def one(d, carry):
        @pl.when(wanted(d))
        def _():
            for theirs, out in zip((1, 0), outs):
                b = b_ref[d, pl.ds(pl.multiple_of(((k + theirs) % 2) * 512, 512), 512), :]
                for r in range(0, 1024, 256):
                    out[r : r + 256, :] += outer(a_ref[d, r : r + 256, :], b)

        return carry

    lax.fori_loop(0, 8, one, 0)


BLOCK = jax.ShapeDtypeStruct((1024, 512), F32)


def block_product(across, down, far):
    ids = range(8) if far else [0, 1, 3, 4, 5, 7]
    n = len(ids)

    def body(*refs):
        a, b = [None] * 8, [None] * 8
        for at, i in enumerate(ids):
            a[i], b[i] = refs[at], refs[n + at]
        block_kernel(far, a, b, refs[2 * n : 2 * n + 2], *refs[2 * n + 2 :])

    return pl.pallas_call(
        body,
        out_shape=(BLOCK, BLOCK),
        in_specs=[pl.BlockSpec(memory_space=pl.ANY)] * (2 * n),
        scratch_shapes=[
            pltpu.VMEM((8, 1024, 512), BF16),
            pltpu.VMEM((8, 1024, 512), BF16),
            pltpu.SemaphoreType.DMA((2, 8)),
        ],
        compiler_params=KERNEL_PARAMS,
        cost_estimate=pl.CostEstimate(flops=4_300_000_000, transcendentals=0, bytes_accessed=14_000_000),
        name="block_far" if far else "block_near",
    )(*[across[i] for i in ids], *[down[i] for i in ids])


def swap(x, axis):
    return lax.ppermute(x, axis, [(0, 1), (1, 0)])


def shift(x, axis, by):
    n = lax.axis_size(axis)
    return lax.ppermute(x, axis, [(i, (i + by) % n) for i in range(n)])


def send(x, axis, src, dst):
    return lax.ppermute(x, axis, [(src, dst)])


def after(x, *others):
    return lax.optimization_barrier((x, *others))[0]


def gather2(x, axis):
    other = swap(x, axis)
    first = lax.axis_index(axis) == 0
    return jnp.stack([jnp.where(first, x, other), jnp.where(first, other, x)])


def ring4(x, axis):
    return [x, shift(x, axis, -1), shift(x, axis, 2), shift(x, axis, 1)]


def in_order(parts, axis):
    size = parts[0].shape[0]
    out = jnp.zeros((4 * size,) + parts[0].shape[1:], parts[0].dtype)
    for step, part in enumerate(parts):
        at = (lax.axis_index(axis) + step) % 4
        out = lax.dynamic_update_slice_in_dim(out, part, at * size, 0)
    return out


def scatter2(x, axis):
    me = lax.axis_index(axis)
    other = swap(lax.dynamic_index_in_dim(x, 1 - me, 0, False), axis)
    return lax.dynamic_index_in_dim(x, me, 0, False) + other


def scatter4(x, axis):
    me = lax.axis_index(axis)
    pick = lambda ahead: lax.dynamic_index_in_dim(x, (me + ahead) % 4, 0, False)
    return (pick(0) + shift(pick(2), axis, 2)) + (shift(pick(1), axis, 1) + shift(pick(3), axis, -1))


def first_of_pair(x):
    return jnp.where(lax.axis_index("xl") == 0, x, send(x, "xl", 0, 1))


def first_of_ring(x):
    return lax.select_n(lax.axis_index("z"), x, send(x, "z", 0, 1), send(x, "z", 0, 2), send(x, "z", 0, 3))


def transpose_chips(x):
    pairs = []
    for d in range(math.prod(SIZES)):
        k, c, r = d % 2, (d // 2) % 8, d // 16
        pairs.append((d, (c * 8 + r) * 2 + k))
    return lax.ppermute(x, AXES, pairs)


def sum_rows(x):
    x = x + swap(x, "xl")
    x = x + lax.ppermute(x, "z", [(i, i ^ 1) for i in range(4)])
    return x + lax.ppermute(x, "z", [(i, i ^ 2) for i in range(4)])


def embed(occupations, table):
    onehot = jnp.concatenate([(occupations == v).astype(F32) for v in range(3)], axis=1)
    embedded = jnp.dot(onehot, table, precision=lax.Precision.HIGH, preferred_element_type=F32)
    return embedded * lax.rsqrt(jnp.mean(embedded * embedded, axis=-1, keepdims=True) + norm_eps)


def log_derivatives(embedded, weights, biases, heads):
    blocks = []
    for p in range(2):
        hidden = jnp.dot(embedded, weights[p], precision=lax.Precision.HIGH, preferred_element_type=F32)
        blocks.append(heads[p] * jax.nn.sigmoid(hidden + biases[p]))
    return jnp.concatenate(blocks, axis=1)


def outer(a, b):
    return lax.dot_general(a, b, (((1,), (1,)), ((), ())), preferred_element_type=F32)


def outer3(a, b):
    return lax.dot_general(
        a, b, (((1,), (1,)), ((), ())), precision=lax.Precision.HIGH, preferred_element_type=F32
    )


def on_device(occupations, table, weights, biases, heads, energies):
    rows = occupations.shape[0]
    total = rows * 8
    cols = total // 16
    z, xl, xh, y, core = [lax.axis_index(a) for a in AXES]
    row, chip_col = z * 2 + xl, xh * 4 + y
    par = weights.shape[0] * weights.shape[2]

    side_parts, remains = [], energies.reshape(-1, occupations.shape[1])
    for _ in range(3):
        rounded = lax.reduce_precision(remains, 8, 7)
        side_parts.append(rounded.astype(BF16))
        remains = remains - rounded
    pair_occ = first_of_pair(jnp.concatenate([occupations.astype(BF16), *side_parts]))
    embedded = embed(occupations, table)
    first_occ = after(first_of_ring(pair_occ), embedded)
    first_side = jnp.sum(first_occ[rows:].astype(F32).reshape(3, rows), axis=0, keepdims=True)
    first_occ = first_occ[:rows]
    derivs = log_derivatives(embedded, weights, biases, heads)
    sums = jnp.sum(derivs, axis=0, keepdims=True)
    first_embedded = embed(after(first_occ, sums), table)
    first_derivs = log_derivatives(first_embedded, weights, biases, heads)
    mean = sum_rows(sums) / total
    center = lambda d: ((d - mean) * (1.0 / math.sqrt(total))).astype(BF16)
    own, first = center(derivs), center(first_derivs)

    eye = lambda r, c, r0, c0: jnp.where(
        (lax.broadcasted_iota(jnp.int32, (r, c), 0) + r0) == (lax.broadcasted_iota(jnp.int32, (r, c), 1) + c0),
        diag_shift,
        0.0,
    ).astype(F32)

    pick = first.reshape(2, 4, 4, 2, 16, par)
    pick = lax.dynamic_index_in_dim(lax.dynamic_index_in_dim(pick, z, 1, False), xl, 2, False)
    slab = outer(pick.reshape(128, par), first).reshape(2, 4, 2, 8, rows)
    own_x = after(own, slab)
    turned = transpose_chips(own_x)
    slab = scatter2(slab, "k")
    panel = outer(own_x, first).reshape(2, 4, 2, rows // 16, rows)
    panel = scatter2(panel, "k")
    slab = scatter4(slab, "y")
    turned_next, turned_prev = shift(turned, "z", -1), shift(turned, "z", 1)
    slab = scatter2(slab, "xh")
    slab = gather2(gather2(slab, "xh"), "xl")
    beside = swap(after(own, slab), "xh")
    turned_side = swap(after(turned, slab), "xl")
    slab = in_order(ring4(slab.reshape(32, rows), "y"), "y")
    panel = scatter4(after(panel, slab), "y")
    own_y = after(own, slab)
    own_next, own_prev = shift(own_y, "y", -1), shift(own_y, "y", 1)
    parts = ring4(slab, "z")
    parts = parts + [swap(p, "k") for p in parts]
    turned_side, beside, *parts = lax.optimization_barrier((turned_side, beside, *parts))
    side_next, side_prev = shift(beside, "y", -1), shift(beside, "y", 1)
    tside_next, tside_prev = (shift(turned_side, "z", -1), shift(turned_side, "z", 1))
    panel = scatter2(after(panel, *parts), "xh")

    low, rest = start_inverse(parts)
    panel, side_next, tside_next, own_prev, turned_prev, rest = lax.optimization_barrier(
        (panel, side_next, tside_next, own_prev, turned_prev, rest)
    )
    mine = gather2(panel, "xh").reshape(rows // 8, rows)
    panel_turned = transpose_chips(panel)
    own_far = shift(own_prev, "y", 1)
    turned_far = shift(turned_prev, "z", 1)
    side_far = shift(side_next, "y", -1)
    tside_far = shift(tside_next, "z", -1)

    mid, rest = go_on_inverse(rest, 256)
    panel_turned, mine, rest = lax.optimization_barrier((panel_turned, mine, rest))
    mine = ring4(mine, "y")
    other = gather2(panel_turned, "xl").reshape(rows // 8, rows)

    (high,) = go_on_inverse(rest, 256)
    other, high = lax.optimization_barrier((other, high))
    other = ring4(other, "z")

    across = [own, own_next, own_far, own_prev, beside, side_next, side_far, side_prev]
    down = [turned, turned_next, turned_far, turned_prev, turned_side, tside_next, tside_far, tside_prev]
    theirs, block = block_product(across, down, False)
    block = block + swap(theirs, "k")
    theirs, last = block_product(across, down, True)
    theirs, *mine = lax.optimization_barrier((theirs, *mine))
    block = (block + last) + swap(theirs, "k")

    mine = gather2(in_order(mine, "y"), "k").reshape(rows, rows)
    other = in_order(other, "z").reshape(2, 4, rows // 16, rows).transpose(1, 0, 2, 3).reshape(cols, rows)
    mine = mine + eye(rows, rows, row * rows, 0)
    other = other + eye(cols, rows, chip_col * rows + core * cols, 0)
    inverse = [low[:, :512], mid[:, :768], high]
    left = jnp.concatenate([outer3(mine[:, : w.shape[1]], w) for w in inverse], 1)
    right = jnp.concatenate([outer3(other[:, : w.shape[1]], w) for w in inverse], 1)
    exact = lambda a, b: lax.dot_general(
        a, b, (((1,), (1,)), ((), ())), precision=lax.Precision.HIGHEST, preferred_element_type=F32
    )
    solved = jnp.concatenate([exact(first_side[:, : w.shape[1]], w) for w in inverse], 1)
    side = energies - jnp.sum(left * solved, axis=1)
    side = jnp.where(row == 0, solved[0], side)
    block = (block + eye(rows, cols, row * rows, chip_col * rows + core * cols)) - outer3(left, right)

    schur = block
    return schur, side


def solution(mesh):
    torus = Mesh(mesh.devices.reshape(SIZES), AXES)
    placed = (P(ROW, None), P(), P(None, None, COL), P(None, COL), P(None, COL), P(ROW))


    return jax.shard_map(on_device, mesh=torus, in_specs=placed, out_specs=(P(ROW, COL), P(ROW)), check_vma=False)
```
